128 devices in a mesh: dp: 4 (over y), ctx: 32 (over x, z, core).
Axes of the slice: x: 4, y: 4, z: 4, core: 2. Of those that a mesh axis runs over, the one named last changes fastest.
Arguments:
- tokens: bfloat16 [32768, 1024], P(('dp', 'ctx')), parts along dimension 0, may hold values from -48 to 48
- w_query: bfloat16 [1024, 1024], replicated
- w_key: bfloat16 [1024, 1024], replicated
- w_value: bfloat16 [1024, 1024], replicated, may hold values from -0.1875 to 0.1875
- w_out: bfloat16 [1024, 1024], replicated, may hold values from -0.5 to 0.5
- norm_gain: float32 [1024], replicated, may hold values from 0.5 to 1.5
- norm_bias: float32 [1024], replicated, may hold values from -4 to 4
- w_pool: bfloat16 [1024, 1024], replicated, may hold values from -0.1875 to 0.1875
- pool_bias: float32 [1024], replicated, may hold values from -6 to 6
- random_ids: int32 [512, 16, 3], P(('dp', 'ctx')), parts along dimension 0, may hold values from 0 to 127, as said below
- lengths: int32 [32], P('dp'), parts along dimension 0, may hold values from 1 to 2048, 8192 in all
Outputs:
- encoded: bfloat16 [32768, 1024], P(('dp', 'ctx')), parts along dimension 0
- doc_vectors: float32 [32, 1024], P('dp'), parts along dimension 0
The draws below stay inside these ranges and needn't reach their ends.
There are 4 independent parts, one for each index of `dp`. The reference program is written for one: setup_inputs(seed, part) draws one part's arguments, and reference() takes and returns one part's arrays. A program takes and returns all parts, laid end to end along the dimension named above; an argument that names none is the same for every part. Nothing has to cross between parts.
Inputs may be any that keep to these rules, and one draw needn't show every extreme that they name: `random_ids`: entry [b, h, r] is the key block of the r-th random block of query block b and head h. Among the 192 entries of the rows of one device, at most 8 name blocks of the range i * 4 to (i + 1) * 4 - 1 of any one device i; in every draw some device's range is named by exactly 8 entries of the rows of every device.
All inputs are finite; a program needn't handle non-finite values.
Results may differ from the reference program's by a relative error of at most 0.0089.
Values may be sent and summed in bfloat16 or wider, within the bound.
A program may use at most 128 MiB of HBM per device.

```python
import math
import jax
import jax.numpy as jnp
import numpy as np
from jax import lax

D = 1024
HEADS = 16
BLK = 64
RAND = 3
DOCS = 8
SHARDS = 32
SEQ = 8192
BPD = 4
NBLK = 128
REQ = 192
CAP = 8
MOST = 2048


def draw_tokens(key, part):
    key_noise = jax.random.fold_in(jax.random.fold_in(key, 5), 0)
    noise = jax.random.normal(key_noise, (SEQ, D), jnp.float32)
    values = noise
    return jnp.clip(values, -48.0, 48.0).astype(jnp.bfloat16)


def query_key_pair(key):
    key_first, key_second = jax.random.split(jax.random.fold_in(key, 11), 2)
    first = jax.random.normal(key_first, (D, D), jnp.float32) / math.sqrt(D)
    second = jax.random.normal(key_second, (D, D), jnp.float32) / math.sqrt(D)
    return (first, second)


def draw_w_query(key, part):
    return query_key_pair(key)[0].astype(jnp.bfloat16)


def draw_w_key(key, part):
    return query_key_pair(key)[1].astype(jnp.bfloat16)


def draw_random_ids(key, part):
    key_hot, key_pool, key_local = jax.random.split(jax.random.fold_in(key, 23), 3)
    hottest = jax.random.randint(key_hot, (), 0, SHARDS)
    others = (hottest + 1 + jnp.arange(SHARDS - 1, dtype=jnp.int32)) % SHARDS
    pool_owners = jnp.repeat(others, CAP)

    def one_source(source_key):
        key_take, key_order = jax.random.split(source_key)
        taken = jax.random.permutation(key_take, pool_owners)[:REQ - CAP]
        owners = jnp.concatenate((jnp.full((CAP,), hottest, jnp.int32), taken.astype(jnp.int32)))
        return jax.random.permutation(key_order, owners)
    owners = jax.vmap(one_source)(jax.random.split(key_pool, SHARDS))
    local_block = jax.random.randint(key_local, (SHARDS, REQ), 0, BPD)
    block_ids = owners * BPD + local_block
    return block_ids.reshape(NBLK, HEADS, RAND).astype(jnp.int32)


def split_up(number_of, total, bound, skew):
    loads = [(1 << 20) // math.isqrt(rank ** skew) + 1 for rank in range(2, number_of + 1)]
    spare, given = total - bound - (number_of - 1), [1] * (number_of - 1)
    while spare > 0:
        free = [i for i in range(number_of - 1) if given[i] < bound]
        whole, remaining = sum([loads[i] for i in free]), spare
        for i in free:
            more = min(bound - given[i], max(1, remaining * loads[i] // whole), spare)
            given[i] = given[i] + more
            spare = spare - more
    return np.array([bound] + given)


def uneven_parts(key, amount, total, bound, skew):
    if amount == 2:
        one = jax.random.randint(key, (), max(1, total - bound), min(bound, total - 1) + 1)
        return jnp.stack([one, total - one])
    tallies = jnp.asarray(split_up(amount, total, bound, skew), jnp.int32)
    twos = (amount - 1) // 2
    donor, receiver = tallies[1:1 + 2 * twos:2], tallies[2:2 + 2 * twos:2]
    slack = jnp.minimum(donor - 1, bound - receiver)
    passed = jax.random.randint(jax.random.fold_in(key, 1), (twos,), 0, 1 << 20) % (slack + 1)
    tallies = tallies.at[1:1 + 2 * twos:2].set(donor - passed).at[2:2 + 2 * twos:2].set(receiver + passed)
    return tallies[jax.random.permutation(jax.random.fold_in(key, 2), amount)]


def gaussian(rng, shape, deviation, limit, kind=jnp.bfloat16):
    entries = deviation * jax.random.normal(rng, shape, jnp.float32)
    return jnp.clip(entries, min=-limit, max=limit).astype(kind)


def setup_inputs(seed: int = 0, part: int = 0) -> dict:
    key_list = jax.random.split(jax.random.key(seed), 12)
    own_keys = jax.random.split(jax.random.fold_in(key_list[11], part), 12)
    tokens = draw_tokens(jax.random.fold_in(jax.random.fold_in(key_list[11], part), 71), part)
    w_query = draw_w_query(jax.random.fold_in(key_list[11], 71), part)
    w_key = draw_w_key(jax.random.fold_in(key_list[11], 71), part)
    w_value = gaussian(key_list[3], (D, D), D ** -0.5, 0.1875)
    w_out = gaussian(key_list[4], (D, D), (D // 8) ** -0.5, 0.5)
    norm_gain = jnp.clip(1.0 + 0.1 * jax.random.normal(key_list[5], (D,), jnp.float32), 0.5, 1.5)
    norm_bias = gaussian(key_list[6], (D,), 0.3, 4.0, jnp.float32)
    w_pool = gaussian(key_list[7], (D, D), D ** -0.5, 0.1875)
    pool_bias = gaussian(key_list[8], (D,), 0.5, 6.0, jnp.float32)
    random_ids = draw_random_ids(jax.random.fold_in(jax.random.fold_in(key_list[11], part), 71), part)
    lengths = uneven_parts(own_keys[10], DOCS, SEQ, MOST, 2).astype(jnp.int32)
    return {"tokens": tokens, "w_query": w_query, "w_key": w_key, "w_value": w_value, "w_out": w_out, "norm_gain": norm_gain, "norm_bias": norm_bias, "w_pool": w_pool, "pool_bias": pool_bias, "random_ids": random_ids, "lengths": lengths}


masked_score = -30000.0

def doc_number(positions, doc_ends):
    return lax.optimization_barrier(jnp.sum((positions[..., None] >= doc_ends).astype(jnp.int32), axis=-1)).astype(jnp.int32)

def partial_attention(queries, keys_in, values_in, query_pos, key_pos, doc_ends, seq_total, by_document):
    score_scale = queries.shape[-1] ** (-0.5)
    scores = jnp.einsum('...qd,...kd->...qk', queries.astype(jnp.float32), keys_in.astype(jnp.float32)) * score_scale
    inside = ((key_pos >= 0) & (key_pos < seq_total))[..., None, :]
    if by_document:
        same_doc = doc_number(query_pos, doc_ends)[..., :, None] == doc_number(key_pos, doc_ends)[..., None, :]
        inside = same_doc & inside
    scores = jnp.where(inside, scores, masked_score)
    row_max = lax.optimization_barrier(jnp.max(scores, axis=-1))
    weights = jnp.exp(scores - row_max[..., None])
    row_total = lax.optimization_barrier(jnp.sum(weights, axis=-1))
    rounded = weights.astype(jnp.bfloat16).astype(jnp.float32)
    partial_out = jnp.einsum('...qk,...kd->...qd', rounded, values_in.astype(jnp.float32))
    return (row_max, row_total, partial_out)

def combine(win_parts, rand_parts):
    win_max, win_total, win_out = win_parts
    rand_max, rand_total, rand_out = rand_parts
    joint_max = jnp.maximum(win_max, lax.optimization_barrier(jnp.max(rand_max, axis=2)))
    win_scale = jnp.exp(win_max - joint_max)
    rand_scale = jnp.exp(rand_max - joint_max[:, :, None])
    numerator = win_scale[..., None] * win_out + lax.optimization_barrier(jnp.sum(rand_scale[..., None] * rand_out, axis=2))
    denominator = win_scale * win_total + lax.optimization_barrier(jnp.sum(rand_scale * rand_total, axis=2))
    return (numerator / denominator[..., None]).astype(jnp.bfloat16)

def head_blocks(rows):
    return rows.reshape(-1, BLK, HEADS, rows.shape[1] // HEADS).transpose(0, 2, 1, 3)

def reference(tokens, w_query, w_key, w_value, w_out, norm_gain, norm_bias, w_pool, pool_bias, random_ids, lengths):
    head_dim = D // HEADS
    doc_ends = jnp.cumsum(lengths).astype(jnp.int32)
    queries = jnp.dot(tokens, w_query, preferred_element_type=jnp.float32).astype(jnp.bfloat16)
    keys_rows = jnp.dot(tokens, w_key, preferred_element_type=jnp.float32).astype(jnp.bfloat16)
    values_rows = jnp.dot(tokens, w_value, preferred_element_type=jnp.float32).astype(jnp.bfloat16)
    query_all = head_blocks(queries)
    keys_all = head_blocks(keys_rows)
    values_all = head_blocks(values_rows)
    zero_block = jnp.zeros((1, HEADS, BLK, head_dim), keys_all.dtype)
    keys_pad = jnp.concatenate((zero_block, keys_all, zero_block), axis=0)
    values_pad = jnp.concatenate((zero_block, values_all, zero_block), axis=0)
    head_index = jnp.arange(HEADS, dtype=jnp.int32)[None, :, None]

    def group(group_index):
        start_block = (group_index * BPD).astype(jnp.int32)
        query_group = lax.dynamic_slice_in_dim(query_all, start_block, BPD, 0)
        keys_group = lax.dynamic_slice_in_dim(keys_pad, start_block, BPD + 2, 0)
        values_group = lax.dynamic_slice_in_dim(values_pad, start_block, BPD + 2, 0)
        window_keys = jnp.concatenate((keys_group[:-2], keys_group[1:-1], keys_group[2:]), axis=2)
        window_values = jnp.concatenate((values_group[:-2], values_group[1:-1], values_group[2:]), axis=2)
        block_ids = start_block + jnp.arange(BPD, dtype=jnp.int32)
        query_pos = block_ids[:, None, None] * BLK + jnp.arange(BLK, dtype=jnp.int32)
        window_pos = (block_ids - 1)[:, None, None] * BLK + jnp.arange(3 * BLK, dtype=jnp.int32)
        win_parts = partial_attention(query_group, window_keys, window_values, query_pos, window_pos, doc_ends, SEQ, True)
        wanted = lax.dynamic_slice_in_dim(random_ids, start_block, BPD, 0)
        rand_keys = keys_all[wanted, head_index]
        rand_values = values_all[wanted, head_index]
        rand_queries = jnp.broadcast_to(query_group[:, :, None], rand_keys.shape)
        rand_pos = (wanted * BLK)[..., None] + jnp.arange(BLK, dtype=jnp.int32)
        rand_parts = partial_attention(rand_queries, rand_keys, rand_values, query_pos[:, :, None], rand_pos, doc_ends, SEQ, False)
        attention = combine(win_parts, rand_parts)
        return attention.transpose(0, 2, 1, 3).reshape(BPD * BLK, D)
    attn_rows = lax.map(group, jnp.arange(SHARDS, dtype=jnp.int32)).reshape(SEQ, D)
    mixed = tokens.astype(jnp.float32) + jnp.dot(attn_rows, w_out, preferred_element_type=jnp.float32)
    centre = lax.optimization_barrier(jnp.mean(mixed, axis=1, keepdims=True))
    spread = lax.optimization_barrier(jnp.mean(jnp.square(mixed - centre), axis=1, keepdims=True))
    encoded = ((mixed - centre) * lax.rsqrt(spread + 1e-05) * norm_gain + norm_bias).astype(jnp.bfloat16)
    starts = (doc_ends - lengths).astype(jnp.int32)
    pooled = encoded[starts]
    doc_vectors = jnp.tanh(jnp.dot(pooled, w_pool, preferred_element_type=jnp.float32) + pool_bias)
    return (encoded, doc_vectors)
```

```python
import jax
import jax.numpy as jnp
from jax import lax
from jax.experimental import pallas as pl
from jax.experimental.pallas import tpu as pltpu
from jax.sharding import PartitionSpec as P

HEADS = 16
BLK = 64
RAND = 3
DOCS = 8
D = 1024
ROWS = 256
SEQ = 8192
NBLK = 128
SIDE = 4
CHIPS = 16
SHARDS = 32
IDS = HEADS * RAND * (ROWS // BLK)
KEYS = 6 * BLK
QROWS = 144

MESH = pl.DeviceIdType.MESH
BF = jnp.bfloat16
F32 = jnp.float32
MASKED = -240000.0
EXP_SCALE = 0.125 * 1.4426950408889634


def turn(a):
    return a + (a // 2) * (1 - 2 * (a % 2))


def kernel(
    ids_ref, len_ref, tok_ref, gain_ref, bias_ref, pbias_ref,
    wq_hbm, wk_hbm, wv_hbm, wo_hbm, wp_hbm,
    enc_ref, doc_ref,
    wq, wk, wv, wo, wp,
    kv_send, kv_buf, q_send, q_recv, att_send, att_recv, doc_send, doc_recv,
    ids_recv, ids_smem, lhs, mixed,
    w_sem, own_sem, ids_ss, ids_rs, kv_ss, kv_rs, sib_ss, sib_rs,
    q_ss, q_rs, att_ss, att_rs, doc_ss, doc_rs,
):
    dp = lax.axis_index("dp")
    me = lax.axis_index("ctx")
    core = me % 2
    chip = me // 2
    cx = chip // SIDE
    cz = chip % SIDE

    def chip_at(k, sign):
        dx, dz = turn(k // SIDE), turn(k % SIDE)
        return ((cx + sign * dx + SIDE) % SIDE) * SIDE + (cz + sign * dz + SIDE) % SIDE

    def to_ctx(c):
        return (dp, 2 * c + core)

    sibling = (dp, 2 * chip + 1 - core)

    barrier = pltpu.get_barrier_semaphore()

    def greet(j, carry):
        pl.semaphore_signal(
            barrier, inc=1, device_id=(dp, (me + j) % SHARDS), device_id_type=MESH
        )
        return carry

    lax.fori_loop(1, SHARDS, greet, 0)

    def load(hbm, vmem, n):
        return pltpu.make_async_copy(hbm, vmem, w_sem.at[n])

    loads = [
        load(wk_hbm, wk, 0), load(wv_hbm, wv, 1), load(wq_hbm, wq, 2),
        load(wo_hbm, wo, 3), load(wp_hbm, wp, 4),
    ]
    for copy in loads:
        copy.start()

    lane = lax.broadcasted_iota(jnp.int32, (1, 128), 1)
    low = lane < 64

    def interleave(first, second):
        return (
            jnp.where(low, first, pltpu.roll(second, 64, 1)),
            jnp.where(low, pltpu.roll(first, 64, 1), second),
        )

    ends, starts = [], []
    total = jnp.int32(0)
    for d in range(DOCS):
        starts.append(total)
        total = total + len_ref[d]
        ends.append(total)

    def rows_of(i):
        return pl.ds(4 * i + 1, 4)

    loads[0].wait()
    loads[1].wait()

    def kv_step(g, carry):
        cols = pl.ds(pl.multiple_of(g * 256, 256), 256)
        k = jnp.dot(tok_ref[...], wk[:, cols], preferred_element_type=F32)
        v = jnp.dot(tok_ref[...], wv[:, cols], preferred_element_type=F32)
        for p in range(2):
            s = slice(128 * p, 128 * p + 128)
            even, odd = interleave(k[:, s], v[:, s])
            kv_send[4 * g + 2 * p] = even.astype(BF).reshape(4, BLK, 128)
            kv_send[4 * g + 2 * p + 1] = odd.astype(BF).reshape(4, BLK, 128)
        return carry

    lax.fori_loop(0, 4, kv_step, 0)

    pl.semaphore_wait(barrier, SHARDS - 1)

    def ids_copy(k):
        return pltpu.make_async_remote_copy(
            src_ref=ids_ref, dst_ref=ids_recv.at[chip], send_sem=ids_ss.at[k],
            recv_sem=ids_rs.at[k], device_id=to_ctx(chip_at(k, 1)), device_id_type=MESH,
        )

    def kv_copy(k):
        c = chip_at(k, 1)
        return pltpu.make_async_remote_copy(
            src_ref=kv_send.at[c], dst_ref=kv_buf.at[rows_of(me)], send_sem=kv_ss.at[k],
            recv_sem=kv_rs.at[k], device_id=to_ctx(c), device_id_type=MESH,
        )

    def q_copy(k):
        c = chip_at(k, 1)
        return pltpu.make_async_remote_copy(
            src_ref=q_send.at[c], dst_ref=q_recv.at[k], send_sem=q_ss.at[k],
            recv_sem=q_rs.at[k], device_id=to_ctx(c), device_id_type=MESH,
        )

    def att_copy(k):
        c = chip_at(k, -1)
        return pltpu.make_async_remote_copy(
            src_ref=att_send.at[c], dst_ref=att_recv.at[chip], send_sem=att_ss.at[k],
            recv_sem=att_rs.at[k], device_id=to_ctx(c), device_id_type=MESH,
        )

    def sib_own():
        return pltpu.make_async_remote_copy(
            src_ref=kv_send.at[chip], dst_ref=kv_buf.at[rows_of(me)],
            send_sem=sib_ss.at[0], recv_sem=sib_rs.at[0], device_id=sibling,
            device_id_type=MESH,
        )

    def sib_copy(k):
        rows = rows_of(2 * chip_at(k, -1) + core)
        return pltpu.make_async_remote_copy(
            src_ref=kv_buf.at[rows], dst_ref=kv_buf.at[rows],
            send_sem=sib_ss.at[k], recv_sem=sib_rs.at[k], device_id=sibling,
            device_id_type=MESH,
        )

    def doc_copy(j):
        return pltpu.make_async_remote_copy(
            src_ref=doc_send, dst_ref=doc_recv.at[me], send_sem=doc_ss.at[j],
            recv_sem=doc_rs.at[j], device_id=(dp, (me + j) % SHARDS), device_id_type=MESH,
        )

    def loop(lo, hi, body):
        def step(k, carry):
            body(k)
            return carry
        lax.fori_loop(lo, hi, step, 0)

    loop(1, CHIPS, lambda k: ids_copy(k).start())
    loop(1, CHIPS, lambda k: kv_copy(k).start())
    sib_own().start()
    own_kv = pltpu.make_async_copy(kv_send.at[chip], kv_buf.at[rows_of(me)], own_sem.at[0])
    own_kv.start()
    own_ids = pltpu.make_async_copy(ids_ref, ids_recv.at[chip], own_sem.at[1])
    own_ids.start()

    first_row = me * ROWS
    pick_row = lax.broadcasted_iota(jnp.int32, (16, 1), 0)
    pick = jnp.full((16, 1), -1, jnp.int32)
    for d in range(DOCS):
        pick = jnp.where(pick_row == d, starts[d], pick)
    pos = first_row + lax.broadcasted_iota(jnp.int32, (1, ROWS), 1)
    chooser = jnp.where(pick == pos, 1.0, 0.0).astype(BF)

    loads[2].wait()

    def q_step(g, carry):
        cols = pl.ds(pl.multiple_of(g * 256, 256), 256)
        q = jnp.dot(tok_ref[...], wq[:, cols], preferred_element_type=F32)
        t = jnp.dot(chooser, tok_ref[:, cols], preferred_element_type=F32)
        for p in range(2):
            s = slice(128 * p, 128 * p + 128)
            even, odd = interleave(q[:128, s], q[128:, s])
            q_send[4 * g + 2 * p, 0:128, :] = even.astype(BF)
            q_send[4 * g + 2 * p + 1, 0:128, :] = odd.astype(BF)
            q_send[4 * g + 2 * p, 128:QROWS, :] = t[:, s].astype(BF)
            q_send[4 * g + 2 * p + 1, 128:QROWS, :] = pltpu.roll(t[:, s], 64, 1).astype(BF)
        return carry

    lax.fori_loop(0, 4, q_step, 0)
    loop(1, CHIPS, lambda k: q_copy(k).start())
    own_q = pltpu.make_async_copy(q_send.at[chip], q_recv.at[0], own_sem.at[2])
    own_q.start()

    kv_buf[0] = jnp.zeros((BLK, 128), BF)
    kv_buf[NBLK + 1] = jnp.zeros((BLK, 128), BF)

    def pass_on(k):
        kv_copy(k).wait_recv()
        sib_copy(k).start()

    loop(1, CHIPS, pass_on)
    loop(1, CHIPS, lambda k: ids_copy(k).wait_recv())
    own_ids.wait()
    to_smem = pltpu.make_async_copy(ids_recv, ids_smem, own_sem.at[3])
    to_smem.start()
    to_smem.wait()
    own_kv.wait()
    sib_own().wait_recv()
    loop(1, CHIPS, lambda k: sib_copy(k).wait_recv())

    col = lax.broadcasted_iota(jnp.int32, (1, KEYS), 1)
    row = lax.broadcasted_iota(jnp.int32, (BLK, 1), 0)

    def doc_of(positions):
        found = jnp.zeros(positions.shape, jnp.int32)
        for d in range(DOCS):
            found = found + jnp.where(positions >= ends[d], 1, 0)
        return found

    def attend(k):
        c = chip_at(k, -1)
        first = (2 * c + core) * (ROWS // BLK)

        @pl.when(k == 0)
        def _():
            own_q.wait()

        @pl.when(k > 0)
        def _():
            q_copy(k).wait_recv()

        for j in range(2):
            outs = []
            pair = q_recv[k, BLK * j:BLK * j + BLK, :].astype(F32)
            for half in range(2):
                block = j + 2 * half
                b = first + block
                q = pltpu.roll(pair, 64, 1) if half else pair
                q = jnp.where(low, q, 0.0).astype(BF)
                parts = [kv_buf[pl.ds(b, 3)].reshape(3 * BLK, 128)]
                for r in range(RAND):
                    at = ids_smem[c, 0, block * HEADS * RAND + chip * RAND + r]
                    parts.append(kv_buf[at + 1])
                kv = jnp.concatenate(parts, axis=0)
                s = lax.dot_general(
                    q, kv, (((1,), (1,)), ((), ())), preferred_element_type=F32
                )
                kpos = (b - 1) * BLK + col
                kdoc = jnp.where((kpos < 0) | (kpos >= SEQ), -1, doc_of(kpos))
                qdoc = doc_of(b * BLK + row)
                keep = (qdoc == kdoc) | (col >= 3 * BLK)
                s = jnp.where(keep, s, MASKED)
                m = jnp.max(s, axis=1, keepdims=True)
                w = jnp.exp2((s - m) * EXP_SCALE)
                l = jnp.sum(w, axis=1, keepdims=True)
                o = jnp.dot(w.astype(BF), kv, preferred_element_type=F32)
                outs.append(o / l)
            att_send[c, 4 * j:4 * j + 4] = jnp.where(
                low, pltpu.roll(outs[0], 64, 1), outs[1]
            ).astype(BF).reshape(4, 16, 128)

        @pl.when(k > 0)
        def _():
            att_copy(k).start()

    loop(0, CHIPS, attend)
    own_att = pltpu.make_async_copy(att_send.at[chip], att_recv.at[chip], own_sem.at[4])
    own_att.start()

    tok_piece = jnp.zeros((16, 128), F32)
    for k in range(CHIPS):
        tok_piece = tok_piece + q_recv[k, 128:QROWS, :].astype(F32)
    att_piece = jnp.zeros((8, 128), F32)
    row8 = lax.broadcasted_iota(jnp.int32, (8, 1), 0)
    row16 = lax.broadcasted_iota(jnp.int32, (16, 1), 0)
    for d in range(DOCS):
        home = starts[d] // ROWS
        local = starts[d] % ROWS
        packed = local % 128
        tile = att_send[home // 2, packed // 16].astype(F32)
        here = row16 + 16 * core == packed % 16 + 16 * (home % 2)
        one = jnp.where(here, tile, 0.0)
        one = jnp.sum(one, axis=0, keepdims=True)
        one = jnp.where(lane * 0 + local >= 128, pltpu.roll(one, 64, 1), one)
        att_piece = jnp.where(row8 == d, one, att_piece)
    doc_send[...] = jnp.concatenate((att_piece, tok_piece[:8]), axis=0).astype(BF)
    loop(1, SHARDS, lambda j: doc_copy(j).start())

    loop(1, CHIPS, lambda k: att_copy(k).wait_recv())
    own_att.wait()
    loads[3].wait()
    for j in range(CHIPS // 2):
        even = att_recv[2 * j].reshape(128, 128).astype(F32)
        odd = att_recv[2 * j + 1].reshape(128, 128).astype(F32)
        top, bottom = interleave(even, odd)
        s = slice(128 * j, 128 * j + 128)
        lhs[0:128, s] = top.astype(BF)
        lhs[128:256, s] = bottom.astype(BF)
    loop(1, SHARDS, lambda j: doc_copy(j).wait_recv())
    doc_recv[me] = doc_send[...]
    pieces = [
        doc_recv[2 * h].astype(F32) + doc_recv[2 * h + 1].astype(F32) for h in range(CHIPS)
    ]
    for j in range(CHIPS // 2):
        both = jnp.where(low, pieces[2 * j], pltpu.roll(pieces[2 * j + 1], 64, 1))
        s = slice(128 * j, 128 * j + 128)
        lhs[256:272, s] = both.astype(BF)
        mixed[256:264, s] = both[8:]
    loads[4].wait()

    def out_step(n, carry):
        cols = pl.ds(pl.multiple_of(n * 256, 256), 256)
        y = jnp.dot(lhs[...], wo[:, cols], preferred_element_type=F32)
        mixed[0:256, cols] = tok_ref[:, cols].astype(F32) + y[:256]
        mixed[256:264, cols] = mixed[256:264, cols] + y[256:264]
        return carry

    lax.fori_loop(0, 4, out_step, 0)

    def normed(rows):
        centre = jnp.mean(rows, axis=1, keepdims=True)
        spread = jnp.mean(jnp.square(rows - centre), axis=1, keepdims=True)
        return ((rows - centre) * lax.rsqrt(spread + 1e-05) * gain_ref[...] + bias_ref[...]).astype(BF)

    def norm_step(n, carry):
        rows = pl.ds(pl.multiple_of(n * 64, 64), 64)
        enc_ref[rows, :] = normed(mixed[rows, :])
        return carry

    lax.fori_loop(0, 4, norm_step, 0)
    pooled = normed(mixed[256:264, :])
    doc_ref[...] = jnp.tanh(
        jnp.dot(pooled, wp[...], preferred_element_type=F32) + pbias_ref[...]
    )

    loop(1, CHIPS, lambda k: ids_copy(k).wait_send())
    loop(1, CHIPS, lambda k: kv_copy(k).wait_send())
    loop(1, CHIPS, lambda k: q_copy(k).wait_send())
    loop(1, CHIPS, lambda k: att_copy(k).wait_send())
    sib_own().wait_send()
    loop(1, CHIPS, lambda k: sib_copy(k).wait_send())
    loop(1, SHARDS, lambda j: doc_copy(j).wait_send())


def per_device(
    tokens, w_query, w_key, w_value, w_out, norm_gain, norm_bias, w_pool, pool_bias,
    random_ids, lengths,
):
    vmem = pl.BlockSpec(memory_space=pltpu.VMEM)
    smem = pl.BlockSpec(memory_space=pltpu.SMEM)
    hbm = pl.BlockSpec(memory_space=pl.ANY)
    ids = jnp.pad(random_ids.reshape(1, IDS), ((0, 0), (0, 256 - IDS)))
    dma = pltpu.SemaphoreType.DMA
    return pl.pallas_call(
        kernel,
        out_shape=(
            jax.ShapeDtypeStruct((ROWS, D), BF),
            jax.ShapeDtypeStruct((DOCS, D), F32),
        ),
        in_specs=[vmem, smem, vmem, vmem, vmem, vmem, hbm, hbm, hbm, hbm, hbm],
        out_specs=(vmem, vmem),
        scratch_shapes=[
            pltpu.VMEM((D, D), BF), pltpu.VMEM((D, D), BF), pltpu.VMEM((D, D), BF),
            pltpu.VMEM((D, D), BF), pltpu.VMEM((D, D), BF),
            pltpu.VMEM((CHIPS, 4, BLK, 128), BF),
            pltpu.VMEM((NBLK + 2, BLK, 128), BF),
            pltpu.VMEM((CHIPS, QROWS, 128), BF),
            pltpu.VMEM((CHIPS, QROWS, 128), BF),
            pltpu.VMEM((CHIPS, 8, 16, 128), BF),
            pltpu.VMEM((CHIPS, 8, 16, 128), BF),
            pltpu.VMEM((16, 128), BF),
            pltpu.VMEM((SHARDS, 16, 128), BF),
            pltpu.VMEM((CHIPS, 1, 256), jnp.int32),
            pltpu.SMEM((CHIPS, 1, 256), jnp.int32),
            pltpu.VMEM((272, D), BF),
            pltpu.VMEM((264, D), F32),
            dma((5,)), dma((5,)),
            dma((CHIPS,)), dma((CHIPS,)), dma((CHIPS,)), dma((CHIPS,)),
            dma((CHIPS,)), dma((CHIPS,)), dma((CHIPS,)), dma((CHIPS,)),
            dma((CHIPS,)), dma((CHIPS,)), dma((SHARDS,)), dma((SHARDS,)),
        ],
        compiler_params=pltpu.CompilerParams(
            collective_id=0, has_side_effects=True, vmem_limit_bytes=56 << 20
        ),
    )(
        ids, lengths, tokens, norm_gain.reshape(1, D), norm_bias.reshape(1, D),
        pool_bias.reshape(1, D), w_query, w_key, w_value, w_out, w_pool,
    )


def solution(mesh):
    rows = P(("dp", "ctx"), None)
    placed = (
        rows, P(), P(), P(), P(), P(), P(), P(), P(),
        P(("dp", "ctx"), None, None), P("dp"),
    )
    return jax.shard_map(
        per_device,
        mesh=mesh,
        in_specs=placed,
        out_specs=(rows, P("dp", None)),
        check_vma=False,
    )
```

```python
import jax
import jax.numpy as jnp
from jax import lax
from jax.experimental import pallas as pl
from jax.experimental.pallas import tpu as pltpu
from jax.sharding import PartitionSpec as P

HEADS = 16
BLK = 64
RAND = 3
DOCS = 8
D = 1024
ROWS = 256
SEQ = 8192
NBLK = 128
SIDE = 4
CHIPS = 16
SHARDS = 32
IDS = HEADS * RAND * (ROWS // BLK)
QROWS = 144
KEYS = 6 * BLK

MESH = pl.DeviceIdType.MESH
BF = jnp.bfloat16
F32 = jnp.float32
MASKED = -240000.0
EXP_SCALE = 0.125 * 1.4426950408889634


ORDER = (0, 1, 3, 2)
STEP = 4
GROUPS = CHIPS // STEP


def turn(a):
    return a + lax.div(a, 2) * (1 - 2 * lax.rem(a, 2))


def kernel(
    ids_ref, len_ref, tok_hbm, gain_ref, bias_ref, pbias_ref,
    wq_hbm, wk_hbm, wv_hbm, wo_hbm, wp_hbm,
    enc_ref, doc_ref,
    tok_ref, wq, wk, wv, wo, wp,
    kv_send, kv_buf, q_send, q_recv, att_send, att_recv, doc_send, doc_recv,
    ids_recv, ids_smem, masks, scores, weights, inverse, lhs, mixed,
    w_sem, own_sem, ids_ss, ids_rs, kv_ss, kv_rs, sib_ss, sib_rs,
    q_ss, q_rs, att_ss, att_rs, doc_ss, doc_rs,
):
    dp = lax.axis_index("dp")
    me = lax.axis_index("ctx")
    core = lax.rem(me, 2)
    chip = lax.div(me, 2)
    cx = lax.div(chip, SIDE)
    cz = lax.rem(chip, SIDE)

    ahead_x = [lax.rem(cx + d, SIDE) for d in ORDER]
    ahead_z = [lax.rem(cz + d, SIDE) for d in ORDER]
    back_x = [lax.rem(cx + SIDE - d, SIDE) for d in ORDER]
    back_z = [lax.rem(cz + SIDE - d, SIDE) for d in ORDER]
    ahead = [x * SIDE + z for x in ahead_x for z in ahead_z]
    back = [x * SIDE + z for x in back_x for z in back_z]

    def to_ctx(c):
        return (dp, 2 * c + core)

    sibling = (dp, 2 * chip + 1 - core)

    barrier = pltpu.get_barrier_semaphore()

    def greet(j, carry):
        pl.semaphore_signal(
            barrier, inc=1, device_id=(dp, lax.rem(me + j, SHARDS)), device_id_type=MESH
        )
        return carry

    def tok_load():
        return pltpu.make_async_copy(tok_hbm, tok_ref, own_sem.at[0])

    def kv_load(g, n):
        cols = pl.ds(pl.multiple_of(g * 256, 256), 256)
        src, dst = ((wk_hbm, wk), (wv_hbm, wv))[n]
        return pltpu.make_async_copy(src.at[:, cols], dst.at[:, cols], w_sem.at[2 * g + n])

    def late_load(n):
        src, dst = ((wq_hbm, wq), (wo_hbm, wo), (wp_hbm, wp))[n]
        return pltpu.make_async_copy(src, dst, w_sem.at[8 + n])

    tok_load().start()
    for g in range(4):
        for n in range(2):
            kv_load(g, n).start()
    for n in range(3):
        late_load(n).start()
    lax.fori_loop(1, SHARDS, greet, 0)

    lane = lax.broadcasted_iota(jnp.int32, (1, 128), 1)
    low = lane < 64

    def interleave(first, second):
        return (
            jnp.where(low, first, pltpu.roll(second, 64, 1)),
            jnp.where(low, pltpu.roll(first, 64, 1), second),
        )

    ends, starts = [], []
    total = jnp.int32(0)
    for d in range(DOCS):
        starts.append(total)
        total = total + len_ref[d]
        ends.append(total)

    def rows_of(i):
        return pl.ds(4 * i + 1, 4)

    tok_load().wait()

    def kv_step(g, carry):
        kv_load(g, 0).wait()
        kv_load(g, 1).wait()
        cols = pl.ds(pl.multiple_of(g * 256, 256), 256)
        k = jnp.dot(tok_ref[...], wk[:, cols], preferred_element_type=F32)
        v = jnp.dot(tok_ref[...], wv[:, cols], preferred_element_type=F32)
        for p in range(2):
            s = slice(128 * p, 128 * p + 128)
            even, odd = interleave(k[:, s], v[:, s])
            kv_send[4 * g + 2 * p] = even.astype(BF).reshape(4, BLK, 128)
            kv_send[4 * g + 2 * p + 1] = odd.astype(BF).reshape(4, BLK, 128)
        return carry

    lax.fori_loop(0, 4, kv_step, 0)

    pl.semaphore_wait(barrier, SHARDS - 1)

    def remote(src, dst, send_sem, recv_sem, device):
        return pltpu.make_async_remote_copy(
            src_ref=src, dst_ref=dst, send_sem=send_sem, recv_sem=recv_sem,
            device_id=device, device_id_type=MESH,
        )

    def ids_copy(k):
        return remote(ids_ref, ids_recv.at[chip], ids_ss, ids_rs, to_ctx(ahead[k]))

    def kv_copy(k):
        return remote(
            kv_send.at[ahead[k]], kv_buf.at[rows_of(me)], kv_ss, kv_rs.at[k], to_ctx(ahead[k])
        )

    def q_copy(k):
        return remote(
            q_send.at[ahead[k]], q_recv.at[k], q_ss, q_rs.at[k // STEP], to_ctx(ahead[k])
        )

    def sib_copy(k):
        rows = rows_of(2 * back[k] + core)
        src = kv_send.at[chip] if k == 0 else kv_buf.at[rows]
        return remote(src, kv_buf.at[rows], sib_ss, sib_rs, sibling)

    def doc_copy(j):
        return remote(doc_send, doc_recv.at[me], doc_ss, doc_rs, (dp, lax.rem(me + j, SHARDS)))

    def drain(ref, sem):
        pltpu.make_async_copy(ref, ref, sem).wait()

    for k in range(1, CHIPS):
        kv_copy(k).start()
    sib_copy(0).start()
    pltpu.make_async_copy(kv_send.at[chip], kv_buf.at[rows_of(me)], own_sem.at[1]).start()

    first_row = me * ROWS
    pick_row = lax.broadcasted_iota(jnp.int32, (16, 1), 0)
    pick = jnp.full((16, 1), -1, jnp.int32)
    for d in range(DOCS):
        pick = jnp.where(pick_row == d, starts[d], pick)
    pos = first_row + lax.broadcasted_iota(jnp.int32, (1, ROWS), 1)
    chooser = jnp.where(pick == pos, 1.0, 0.0).astype(BF)

    late_load(0).wait()

    def q_step(g, carry):
        cols = pl.ds(pl.multiple_of(g * 256, 256), 256)
        q = jnp.dot(tok_ref[...], wq[:, cols], preferred_element_type=F32)
        t = jnp.dot(chooser, tok_ref[:, cols], preferred_element_type=F32)
        for p in range(2):
            s = slice(128 * p, 128 * p + 128)
            even, odd = interleave(q[:128, s], q[128:, s])
            q_send[4 * g + 2 * p, 0:128, :] = even.astype(BF)
            q_send[4 * g + 2 * p + 1, 0:128, :] = odd.astype(BF)
            q_send[4 * g + 2 * p, 128:QROWS, :] = t[:, s].astype(BF)
            q_send[4 * g + 2 * p + 1, 128:QROWS, :] = pltpu.roll(t[:, s], 64, 1).astype(BF)
        return carry

    lax.fori_loop(0, 4, q_step, 0)
    for k in range(1, CHIPS):
        ids_copy(k).start()
    pltpu.make_async_copy(ids_ref, ids_recv.at[chip], ids_rs).start()
    for k in range(1, CHIPS):
        q_copy(k).start()
    pltpu.make_async_copy(q_send.at[chip], q_recv.at[0], q_rs.at[0]).start()

    kv_buf[0] = jnp.zeros((BLK, 128), BF)
    kv_buf[NBLK + 1] = jnp.zeros((BLK, 128), BF)

    col = lax.broadcasted_iota(jnp.int32, (1, 256), 1)
    diagonal = (
        lax.broadcasted_iota(jnp.int32, (BLK, 128), 1)
        == lax.broadcasted_iota(jnp.int32, (BLK, 128), 0) + BLK
    )

    def make_masks(k):
        first = (2 * back[k] + core) * (ROWS // BLK)
        for block in range(4):
            kpos = (first + block - 1) * BLK + col
            kdoc = jnp.zeros((1, 256), F32)
            for d in range(DOCS):
                kdoc = kdoc + jnp.where(kpos >= ends[d], 1.0, 0.0)
            kdoc = jnp.where((kpos < 0) | (kpos >= SEQ), -1.0, kdoc)
            qdoc = jnp.sum(jnp.where(diagonal, kdoc[:, :128], 0.0), axis=1, keepdims=True)
            keep = (qdoc == kdoc) | (col >= 3 * BLK)
            masks[4 * k + block] = jnp.where(keep, 1, 0)

    make_masks(0)
    for k in range(1, CHIPS):
        make_masks(k)
        kv_copy(k).wait_recv()
        sib_copy(k).start()
    drain(ids_recv, ids_rs)
    to_smem = pltpu.make_async_copy(ids_recv, ids_smem, own_sem.at[3])
    to_smem.start()
    to_smem.wait()
    drain(kv_send.at[0], own_sem.at[1])
    drain(kv_send, sib_rs)

    def attend(g, carry):
        drain(q_recv.at[pl.ds(0, STEP)], q_rs.at[g])
        homes = []
        for i in range(STEP):
            k = g * STEP + i
            dx, dz = turn(lax.div(k, SIDE)), turn(lax.rem(k, SIDE))
            x = lax.rem(cx + SIDE - dx, SIDE)
            homes.append(x * SIDE + lax.rem(cz + SIDE - dz, SIDE))

        def keys_of(i, block):
            c = homes[i]
            b = (2 * c + core) * (ROWS // BLK) + block
            parts = [kv_buf[pl.ds(b, 3)].reshape(3 * BLK, 128)]
            for r in range(RAND):
                at = ids_smem[c, 0, block * HEADS * RAND + chip * RAND + r]
                parts.append(kv_buf[at + 1])
            return jnp.concatenate(parts, axis=0)

        def score(i):
            for j in range(2):
                pair = q_recv[g * STEP + i, BLK * j:BLK * j + BLK, :].astype(F32)
                for half in range(2):
                    block = j + 2 * half
                    q = pltpu.roll(pair, 64, 1) if half else pair
                    q = jnp.where(low, q, 0.0).astype(BF)
                    scores[4 * i + block] = lax.dot_general(
                        q, keys_of(i, block), (((1,), (1,)), ((), ())),
                        preferred_element_type=F32,
                    )

        def soften(i):
            for block in range(4):
                t = 4 * i + block
                keep = masks[4 * (g * STEP + i) + block] > 0
                s0 = jnp.where(keep, scores[t, :, 0:256], MASKED)
                s1 = scores[t, :, 256:KEYS]
                m = jnp.maximum(jnp.maximum(s0[:, :128], s0[:, 128:]), s1)
                m = jnp.max(m, axis=1, keepdims=True)
                w0 = jnp.exp2((s0 - m) * EXP_SCALE)
                w1 = jnp.exp2((s1 - m) * EXP_SCALE)
                weights[t, :, 0:256] = w0.astype(BF)
                weights[t, :, 256:KEYS] = w1.astype(BF)
                l = jnp.sum(w0[:, :128] + w0[:, 128:] + w1, axis=1, keepdims=True)
                inverse[t] = jnp.broadcast_to(1.0 / l, (BLK, 128))

        def gather(i):
            for j in range(2):
                outs = []
                for half in range(2):
                    t = 4 * i + j + 2 * half
                    o = jnp.dot(
                        weights[t], keys_of(i, j + 2 * half), preferred_element_type=F32
                    )
                    outs.append(o * inverse[t])
                att_send[homes[i], 4 * j:4 * j + 4] = jnp.where(
                    low, pltpu.roll(outs[0], 64, 1), outs[1]
                ).astype(BF).reshape(4, 16, 128)

        for i in range(STEP + 2):
            if i < STEP:
                score(i)
            if 1 <= i <= STEP:
                soften(i - 1)
            if i >= 2:
                gather(i - 2)

        for i in range(STEP):
            c = homes[i]

            def send(c=c):
                remote(
                    att_send.at[c], att_recv.at[chip], att_ss, att_rs.at[g], to_ctx(c)
                ).start()

            if i == 0:
                pl.when(g > 0)(send)
            else:
                send()
        return carry

    lax.fori_loop(0, GROUPS, attend, 0)
    pltpu.make_async_copy(att_send.at[chip], att_recv.at[chip], att_rs.at[0]).start()

    tok_piece = jnp.zeros((16, 128), F32)
    for k in range(CHIPS):
        tok_piece = tok_piece + q_recv[k, 128:QROWS, :].astype(F32)
    att_piece = jnp.zeros((8, 128), F32)
    row8 = lax.broadcasted_iota(jnp.int32, (8, 1), 0)
    row16 = lax.broadcasted_iota(jnp.int32, (16, 1), 0)
    for d in range(DOCS):
        home = lax.div(starts[d], ROWS)
        local = lax.rem(starts[d], ROWS)
        packed = lax.rem(local, 128)
        tile = att_send[lax.div(home, 2), lax.div(packed, 16)].astype(F32)
        here = row16 + 16 * core == lax.rem(packed, 16) + 16 * lax.rem(home, 2)
        one = jnp.where(here, tile, 0.0)
        one = jnp.sum(one, axis=0, keepdims=True)
        one = jnp.where(lane * 0 + local >= 128, pltpu.roll(one, 64, 1), one)
        att_piece = jnp.where(row8 == d, one, att_piece)
    doc_send[...] = jnp.concatenate((att_piece, tok_piece[:8]), axis=0).astype(BF)
    for j in range(1, SHARDS):
        doc_copy(j).start()
    pltpu.make_async_copy(doc_send, doc_recv.at[me], doc_rs).start()

    late_load(1).wait()
    for g in range(4):
        drain(att_recv.at[pl.ds(0, 4)], att_rs.at[g])
        x = ahead_x[g]
        for p in range(2):
            even = att_recv[4 * x + 2 * p].reshape(128, 128).astype(F32)
            odd = att_recv[4 * x + 2 * p + 1].reshape(128, 128).astype(F32)
            top, bottom = interleave(even, odd)
            s = slice(128 * p, 128 * p + 128)
            lhs[0:128, s] = top.astype(BF)
            lhs[128:256, s] = bottom.astype(BF)
        if g == 3:
            drain(doc_recv, doc_rs)
        heads = pl.ds(pl.multiple_of(x * 256, 256), 256)
        y = jnp.dot(lhs[...], wo[heads, :], preferred_element_type=F32)
        if g == 0:
            mixed[...] = tok_ref[...].astype(F32) + y
        else:
            mixed[...] = mixed[...] + y

    pieces = [
        doc_recv[2 * h].astype(F32) + doc_recv[2 * h + 1].astype(F32) for h in range(CHIPS)
    ]
    opened = jnp.concatenate(
        [
            jnp.where(low, pieces[2 * j], pltpu.roll(pieces[2 * j + 1], 64, 1))
            for j in range(CHIPS // 2)
        ],
        axis=1,
    )
    y = jnp.dot(opened.astype(BF), wo[...], preferred_element_type=F32)
    opened_mixed = opened[8:] + y[:8]

    def normed(rows):
        centre = jnp.mean(rows, axis=1, keepdims=True)
        spread = jnp.mean(jnp.square(rows - centre), axis=1, keepdims=True)
        return ((rows - centre) * lax.rsqrt(spread + 1e-05) * gain_ref[...] + bias_ref[...]).astype(BF)

    def norm_step(n, carry):
        rows = pl.ds(pl.multiple_of(n * 64, 64), 64)
        enc_ref[rows, :] = normed(mixed[rows, :])
        return carry

    lax.fori_loop(0, 4, norm_step, 0)
    late_load(2).wait()
    doc_ref[...] = jnp.tanh(
        jnp.dot(normed(opened_mixed), wp[...], preferred_element_type=F32) + pbias_ref[...]
    )

    others = pl.ds(0, CHIPS - 1)
    drain(ids_recv.at[others], ids_ss)
    drain(kv_send.at[others], kv_ss)
    drain(q_send.at[others], q_ss)
    drain(att_send.at[others], att_ss)
    drain(kv_send, sib_ss)
    drain(doc_recv.at[pl.ds(0, SHARDS - 1)], doc_ss)


def per_device(
    tokens, w_query, w_key, w_value, w_out, norm_gain, norm_bias, w_pool, pool_bias,
    random_ids, lengths,
):
    vmem = pl.BlockSpec(memory_space=pltpu.VMEM)
    smem = pl.BlockSpec(memory_space=pltpu.SMEM)
    hbm = pl.BlockSpec(memory_space=pl.ANY)
    ids = jnp.pad(random_ids.reshape(1, IDS), ((0, 0), (0, 256 - IDS)))
    dma = pltpu.SemaphoreType.DMA
    return pl.pallas_call(
        kernel,
        out_shape=(
            jax.ShapeDtypeStruct((ROWS, D), BF),
            jax.ShapeDtypeStruct((DOCS, D), F32),
        ),
        in_specs=[vmem, smem, hbm, vmem, vmem, vmem, hbm, hbm, hbm, hbm, hbm],
        out_specs=(vmem, vmem),
        scratch_shapes=[
            pltpu.VMEM((ROWS, D), BF),
            pltpu.VMEM((D, D), BF), pltpu.VMEM((D, D), BF), pltpu.VMEM((D, D), BF),
            pltpu.VMEM((D, D), BF), pltpu.VMEM((D, D), BF),
            pltpu.VMEM((CHIPS, 4, BLK, 128), BF),
            pltpu.VMEM((NBLK + 2, BLK, 128), BF),
            pltpu.VMEM((CHIPS, QROWS, 128), BF),
            pltpu.VMEM((CHIPS, QROWS, 128), BF),
            pltpu.VMEM((CHIPS, 8, 16, 128), BF),
            pltpu.VMEM((CHIPS, 8, 16, 128), BF),
            pltpu.VMEM((16, 128), BF),
            pltpu.VMEM((SHARDS, 16, 128), BF),
            pltpu.VMEM((CHIPS, 1, 256), jnp.int32),
            pltpu.SMEM((CHIPS, 1, 256), jnp.int32),
            pltpu.VMEM((CHIPS * 4, BLK, 256), jnp.int32),
            pltpu.VMEM((4 * STEP, BLK, KEYS), F32),
            pltpu.VMEM((4 * STEP, BLK, KEYS), BF),
            pltpu.VMEM((4 * STEP, BLK, 128), F32),
            pltpu.VMEM((ROWS, 256), BF),
            pltpu.VMEM((ROWS, D), F32),
            dma((11,)), dma((4,)), dma, dma, dma, dma((CHIPS,)), dma, dma,
            dma, dma((GROUPS,)), dma, dma((GROUPS,)), dma, dma,
        ],
        compiler_params=pltpu.CompilerParams(
            collective_id=0, has_side_effects=True, vmem_limit_bytes=56 << 20
        ),
    )(
        ids, lengths, tokens, norm_gain.reshape(1, D), norm_bias.reshape(1, D),
        pool_bias.reshape(1, D), w_query, w_key, w_value, w_out, w_pool,
    )


def solution(mesh):
    rows = P(("dp", "ctx"), None)
    placed = (
        rows, P(), P(), P(), P(), P(), P(), P(), P(),
        P(("dp", "ctx"), None, None), P("dp"),
    )
    return jax.shard_map(
        per_device,
        mesh=mesh,
        in_specs=placed,
        out_specs=(rows, P("dp", None)),
        check_vma=False,
    )
```

```python
import jax
import jax.numpy as jnp
from jax import lax
from jax.experimental import pallas as pl
from jax.experimental.pallas import tpu as pltpu
from jax.sharding import PartitionSpec as P

HEADS = 16
BLK = 64
RAND = 3
DOCS = 8
D = 1024
ROWS = 256
SEQ = 8192
NBLK = 128
SIDE = 4
CHIPS = 16
SHARDS = 32
QROWS = 144
KEYS = 6 * BLK

MESH = pl.DeviceIdType.MESH
BF = jnp.bfloat16
F32 = jnp.float32
MASKED = -240000.0
EXP_SCALE = 0.125 * 1.4426950408889634


ORDER = (0, 1, 3, 2)
STEP = 4
GROUPS = CHIPS // STEP


def turn(a):
    return a + lax.div(a, 2) * (1 - 2 * lax.rem(a, 2))


def kernel(
    ids_hbm, len_hbm, tok_hbm, gain_hbm, bias_hbm, pbias_hbm,
    wq_hbm, wk_hbm, wv_hbm, wo_hbm, wp_hbm,
    enc_ref, doc_ref,
    ids_ref, len_ref, tok_ref, gain_ref, bias_ref, pbias_ref, wq, wk, wv, wo, wp,
    kv_send, kv_buf, q_send, q_recv, att_send, att_recv, doc_send, doc_recv,
    ids_recv, ids_smem, masks, scores, weights, inverse, lhs, mixed,
    w_sem, own_sem, ids_ss, ids_rs, kv_ss, kv_rs, sib_ss, sib_rs,
    q_ss, q_rs, att_ss, att_rs, doc_ss, doc_rs,
):
    dp = lax.axis_index("dp")
    me = lax.axis_index("ctx")
    core = lax.rem(me, 2)
    chip = lax.div(me, 2)
    cx = lax.div(chip, SIDE)
    cz = lax.rem(chip, SIDE)

    ahead_x = [lax.rem(cx + d, SIDE) for d in ORDER]
    ahead_z = [lax.rem(cz + d, SIDE) for d in ORDER]
    back_x = [lax.rem(cx + SIDE - d, SIDE) for d in ORDER]
    back_z = [lax.rem(cz + SIDE - d, SIDE) for d in ORDER]
    ahead = [x * SIDE + z for x in ahead_x for z in ahead_z]
    back = [x * SIDE + z for x in back_x for z in back_z]

    def to_ctx(c):
        return (dp, 2 * c + core)

    sibling = (dp, 2 * chip + 1 - core)

    barrier = pltpu.get_barrier_semaphore()

    def greet(j, carry):
        pl.semaphore_signal(
            barrier, inc=1, device_id=(dp, lax.rem(me + j, SHARDS)), device_id_type=MESH
        )
        return carry

    def tok_load():
        return pltpu.make_async_copy(tok_hbm, tok_ref, own_sem.at[0])

    def kv_load(g, n):
        cols = pl.ds(pl.multiple_of(g * 256, 256), 256)
        src, dst = ((wk_hbm, wk), (wv_hbm, wv))[n]
        return pltpu.make_async_copy(src.at[:, cols], dst.at[:, cols], w_sem.at[2 * g + n])

    def late_load(n):
        src, dst = ((wq_hbm, wq), (wo_hbm, wo), (wp_hbm, wp))[n]
        return pltpu.make_async_copy(src, dst, w_sem.at[8 + n])

    def small_load(n):
        src, dst = (
            (len_hbm, len_ref), (ids_hbm, ids_ref), (gain_hbm, gain_ref),
            (bias_hbm, bias_ref), (pbias_hbm, pbias_ref),
        )[n]
        return pltpu.make_async_copy(src, dst, own_sem.at[4 + n])

    tok_load().start()
    for g in range(4):
        for n in range(2):
            kv_load(g, n).start()
    for n in range(5):
        small_load(n).start()
    for n in range(3):
        late_load(n).start()
    lax.fori_loop(1, SHARDS, greet, 0)

    lane = lax.broadcasted_iota(jnp.int32, (1, 128), 1)
    low = lane < 64

    def interleave(first, second):
        return (
            jnp.where(low, first, pltpu.roll(second, 64, 1)),
            jnp.where(low, pltpu.roll(first, 64, 1), second),
        )

    def rows_of(i):
        return pl.ds(4 * i + 1, 4)

    tok_load().wait()

    def kv_step(g, carry):
        kv_load(g, 0).wait()
        kv_load(g, 1).wait()
        cols = pl.ds(pl.multiple_of(g * 256, 256), 256)
        k = jnp.dot(tok_ref[...], wk[:, cols], preferred_element_type=F32)
        v = jnp.dot(tok_ref[...], wv[:, cols], preferred_element_type=F32)
        for p in range(2):
            s = slice(128 * p, 128 * p + 128)
            even, odd = interleave(k[:, s], v[:, s])
            kv_send[4 * g + 2 * p] = even.astype(BF).reshape(4, BLK, 128)
            kv_send[4 * g + 2 * p + 1] = odd.astype(BF).reshape(4, BLK, 128)
        return carry

    lax.fori_loop(0, 4, kv_step, 0)

    pl.semaphore_wait(barrier, SHARDS - 1)

    def remote(src, dst, send_sem, recv_sem, device):
        return pltpu.make_async_remote_copy(
            src_ref=src, dst_ref=dst, send_sem=send_sem, recv_sem=recv_sem,
            device_id=device, device_id_type=MESH,
        )

    def ids_copy(k):
        return remote(ids_ref, ids_recv.at[chip], ids_ss, ids_rs, to_ctx(ahead[k]))

    def kv_copy(k):
        return remote(
            kv_send.at[ahead[k]], kv_buf.at[rows_of(me)], kv_ss, kv_rs.at[k], to_ctx(ahead[k])
        )

    def q_copy(k):
        return remote(
            q_send.at[ahead[k]], q_recv.at[k], q_ss, q_rs.at[k // STEP], to_ctx(ahead[k])
        )

    def sib_copy(k):
        rows = rows_of(2 * back[k] + core)
        src = kv_send.at[chip] if k == 0 else kv_buf.at[rows]
        return remote(src, kv_buf.at[rows], sib_ss, sib_rs, sibling)

    def doc_copy(j):
        return remote(doc_send, doc_recv.at[me], doc_ss, doc_rs, (dp, lax.rem(me + j, SHARDS)))

    def drain(ref, sem):
        pltpu.make_async_copy(ref, ref, sem).wait()

    for k in range(1, CHIPS):
        kv_copy(k).start()
    sib_copy(0).start()
    pltpu.make_async_copy(kv_send.at[chip], kv_buf.at[rows_of(me)], own_sem.at[1]).start()

    small_load(0).wait()
    ends, starts = [], []
    total = jnp.int32(0)
    for d in range(DOCS):
        starts.append(total)
        total = total + len_ref[d]
        ends.append(total)

    first_row = me * ROWS
    pick_row = lax.broadcasted_iota(jnp.int32, (16, 1), 0)
    pick = jnp.full((16, 1), -1, jnp.int32)
    for d in range(DOCS):
        pick = jnp.where(pick_row == d, starts[d], pick)
    pos = first_row + lax.broadcasted_iota(jnp.int32, (1, ROWS), 1)
    chooser = jnp.where(pick == pos, 1.0, 0.0).astype(BF)

    late_load(0).wait()

    def q_step(g, carry):
        cols = pl.ds(pl.multiple_of(g * 256, 256), 256)
        q = jnp.dot(tok_ref[...], wq[:, cols], preferred_element_type=F32)
        t = jnp.dot(chooser, tok_ref[:, cols], preferred_element_type=F32)
        for p in range(2):
            s = slice(128 * p, 128 * p + 128)
            even, odd = interleave(q[:128, s], q[128:, s])
            q_send[4 * g + 2 * p, 0:128, :] = even.astype(BF)
            q_send[4 * g + 2 * p + 1, 0:128, :] = odd.astype(BF)
            q_send[4 * g + 2 * p, 128:QROWS, :] = t[:, s].astype(BF)
            q_send[4 * g + 2 * p + 1, 128:QROWS, :] = pltpu.roll(t[:, s], 64, 1).astype(BF)
        return carry

    lax.fori_loop(0, 4, q_step, 0)
    small_load(1).wait()
    for k in range(1, CHIPS):
        ids_copy(k).start()
    pltpu.make_async_copy(ids_ref, ids_recv.at[chip], ids_rs).start()
    for k in range(1, CHIPS):
        q_copy(k).start()
    pltpu.make_async_copy(q_send.at[chip], q_recv.at[0], q_rs.at[0]).start()

    kv_buf[0] = jnp.zeros((BLK, 128), BF)
    kv_buf[NBLK + 1] = jnp.zeros((BLK, 128), BF)

    col = lax.broadcasted_iota(jnp.int32, (1, 256), 1)
    diagonal = (
        lax.broadcasted_iota(jnp.int32, (BLK, 128), 1)
        == lax.broadcasted_iota(jnp.int32, (BLK, 128), 0) + BLK
    )

    def make_masks(k):
        first = (2 * back[k] + core) * (ROWS // BLK)
        for block in range(4):
            kpos = (first + block - 1) * BLK + col
            kdoc = jnp.zeros((1, 256), F32)
            for d in range(DOCS):
                kdoc = kdoc + jnp.where(kpos >= ends[d], 1.0, 0.0)
            kdoc = jnp.where((kpos < 0) | (kpos >= SEQ), -1.0, kdoc)
            qdoc = jnp.sum(jnp.where(diagonal, kdoc[:, :128], 0.0), axis=1, keepdims=True)
            keep = (qdoc == kdoc) | (col >= 3 * BLK)
            masks[4 * k + block] = jnp.where(keep, 1, 0)

    make_masks(0)
    for k in range(1, CHIPS):
        make_masks(k)
        kv_copy(k).wait_recv()
        sib_copy(k).start()
    drain(ids_recv, ids_rs)
    to_smem = pltpu.make_async_copy(ids_recv, ids_smem, own_sem.at[3])
    to_smem.start()
    to_smem.wait()
    drain(kv_send.at[0], own_sem.at[1])
    drain(kv_send, sib_rs)

    def attend(g, carry):
        drain(q_recv.at[pl.ds(0, STEP)], q_rs.at[g])
        homes = []
        for i in range(STEP):
            k = g * STEP + i
            dx, dz = turn(lax.div(k, SIDE)), turn(lax.rem(k, SIDE))
            x = lax.rem(cx + SIDE - dx, SIDE)
            homes.append(x * SIDE + lax.rem(cz + SIDE - dz, SIDE))

        def keys_of(i, block):
            c = homes[i]
            b = (2 * c + core) * (ROWS // BLK) + block
            parts = [kv_buf[pl.ds(b, 3)].reshape(3 * BLK, 128)]
            for r in range(RAND):
                at = ids_smem[c, r, block, chip]
                parts.append(kv_buf[at + 1])
            return jnp.concatenate(parts, axis=0)

        def score(i):
            for j in range(2):
                pair = q_recv[g * STEP + i, BLK * j:BLK * j + BLK, :].astype(F32)
                for half in range(2):
                    block = j + 2 * half
                    q = pltpu.roll(pair, 64, 1) if half else pair
                    q = jnp.where(low, q, 0.0).astype(BF)
                    scores[4 * i + block] = lax.dot_general(
                        q, keys_of(i, block), (((1,), (1,)), ((), ())),
                        preferred_element_type=F32,
                    )

        def soften(i):
            for block in range(4):
                t = 4 * i + block
                keep = masks[4 * (g * STEP + i) + block] > 0
                s0 = jnp.where(keep, scores[t, :, 0:256], MASKED)
                s1 = scores[t, :, 256:KEYS]
                m = jnp.maximum(jnp.maximum(s0[:, :128], s0[:, 128:]), s1)
                m = jnp.max(m, axis=1, keepdims=True)
                w0 = jnp.exp2((s0 - m) * EXP_SCALE)
                w1 = jnp.exp2((s1 - m) * EXP_SCALE)
                weights[t, :, 0:256] = w0.astype(BF)
                weights[t, :, 256:KEYS] = w1.astype(BF)
                l = jnp.sum(w0[:, :128] + w0[:, 128:] + w1, axis=1, keepdims=True)
                inverse[t] = jnp.broadcast_to(1.0 / l, (BLK, 128))

        def gather(i):
            for j in range(2):
                outs = []
                for half in range(2):
                    t = 4 * i + j + 2 * half
                    o = jnp.dot(
                        weights[t], keys_of(i, j + 2 * half), preferred_element_type=F32
                    )
                    outs.append(o * inverse[t])
                att_send[homes[i], 4 * j:4 * j + 4] = jnp.where(
                    low, pltpu.roll(outs[0], 64, 1), outs[1]
                ).astype(BF).reshape(4, 16, 128)

        for i in range(STEP + 2):
            if i < STEP:
                score(i)
            if 1 <= i <= STEP:
                soften(i - 1)
            if i >= 2:
                gather(i - 2)

        for i in range(STEP):
            c = homes[i]

            def send(c=c):
                remote(
                    att_send.at[c], att_recv.at[chip], att_ss, att_rs.at[g], to_ctx(c)
                ).start()

            if i == 0:
                pl.when(g > 0)(send)
            else:
                send()
        return carry

    lax.fori_loop(0, GROUPS, attend, 0)
    pltpu.make_async_copy(att_send.at[chip], att_recv.at[chip], att_rs.at[0]).start()

    tok_piece = jnp.zeros((16, 128), F32)
    for k in range(CHIPS):
        tok_piece = tok_piece + q_recv[k, 128:QROWS, :].astype(F32)
    att_piece = jnp.zeros((8, 128), F32)
    row8 = lax.broadcasted_iota(jnp.int32, (8, 1), 0)
    row16 = lax.broadcasted_iota(jnp.int32, (16, 1), 0)
    for d in range(DOCS):
        home = lax.div(starts[d], ROWS)
        local = lax.rem(starts[d], ROWS)
        packed = lax.rem(local, 128)
        tile = att_send[lax.div(home, 2), lax.div(packed, 16)].astype(F32)
        here = row16 + 16 * core == lax.rem(packed, 16) + 16 * lax.rem(home, 2)
        one = jnp.where(here, tile, 0.0)
        one = jnp.sum(one, axis=0, keepdims=True)
        one = jnp.where(lane * 0 + local >= 128, pltpu.roll(one, 64, 1), one)
        att_piece = jnp.where(row8 == d, one, att_piece)
    doc_send[...] = jnp.concatenate((att_piece, tok_piece[:8]), axis=0).astype(BF)
    for j in range(1, SHARDS):
        doc_copy(j).start()
    pltpu.make_async_copy(doc_send, doc_recv.at[me], doc_rs).start()

    late_load(1).wait()
    for g in range(4):
        drain(att_recv.at[pl.ds(0, 4)], att_rs.at[g])
        x = ahead_x[g]
        for p in range(2):
            even = att_recv[4 * x + 2 * p].reshape(128, 128).astype(F32)
            odd = att_recv[4 * x + 2 * p + 1].reshape(128, 128).astype(F32)
            top, bottom = interleave(even, odd)
            s = slice(128 * p, 128 * p + 128)
            lhs[0:128, s] = top.astype(BF)
            lhs[128:256, s] = bottom.astype(BF)
        if g == 3:
            drain(doc_recv, doc_rs)
        heads = pl.ds(pl.multiple_of(x * 256, 256), 256)
        y = jnp.dot(lhs[...], wo[heads, :], preferred_element_type=F32)
        if g == 0:
            mixed[...] = tok_ref[...].astype(F32) + y
        else:
            mixed[...] = mixed[...] + y

    pieces = [
        doc_recv[2 * h].astype(F32) + doc_recv[2 * h + 1].astype(F32) for h in range(CHIPS)
    ]
    opened = jnp.concatenate(
        [
            jnp.where(low, pieces[2 * j], pltpu.roll(pieces[2 * j + 1], 64, 1))
            for j in range(CHIPS // 2)
        ],
        axis=1,
    )
    y = jnp.dot(opened.astype(BF), wo[...], preferred_element_type=F32)
    opened_mixed = opened[8:] + y[:8]

    def normed(rows):
        centre = jnp.mean(rows, axis=1, keepdims=True)
        spread = jnp.mean(jnp.square(rows - centre), axis=1, keepdims=True)
        return ((rows - centre) * lax.rsqrt(spread + 1e-05) * gain_ref[...] + bias_ref[...]).astype(BF)

    for n in range(2, 5):
        small_load(n).wait()

    def norm_step(n, carry):
        rows = pl.ds(pl.multiple_of(n * 64, 64), 64)
        enc_ref[rows, :] = normed(mixed[rows, :])
        return carry

    lax.fori_loop(0, 4, norm_step, 0)
    late_load(2).wait()
    doc_ref[...] = jnp.tanh(
        jnp.dot(normed(opened_mixed), wp[...], preferred_element_type=F32) + pbias_ref[...]
    )

    others = pl.ds(0, CHIPS - 1)
    drain(ids_recv.at[others], ids_ss)
    drain(kv_send.at[others], kv_ss)
    drain(q_send.at[others], q_ss)
    drain(att_send.at[others], att_ss)
    drain(kv_send, sib_ss)
    drain(doc_recv.at[pl.ds(0, SHARDS - 1)], doc_ss)


def per_device(
    tokens, w_query, w_key, w_value, w_out, norm_gain, norm_bias, w_pool, pool_bias,
    random_ids, lengths,
):
    vmem = pl.BlockSpec(memory_space=pltpu.VMEM)
    hbm = pl.BlockSpec(memory_space=pltpu.HBM)
    ids = random_ids.transpose(2, 0, 1)
    dma = pltpu.SemaphoreType.DMA
    return pl.pallas_call(
        kernel,
        out_shape=(
            jax.ShapeDtypeStruct((ROWS, D), BF),
            jax.ShapeDtypeStruct((DOCS, D), F32),
        ),
        in_specs=[hbm] * 11,
        out_specs=(vmem, vmem),
        scratch_shapes=[
            pltpu.VMEM((RAND, 4, HEADS), jnp.int32), pltpu.SMEM((DOCS,), jnp.int32),
            pltpu.VMEM((ROWS, D), BF),
            pltpu.VMEM((1, D), F32), pltpu.VMEM((1, D), F32), pltpu.VMEM((1, D), F32),
            pltpu.VMEM((D, D), BF), pltpu.VMEM((D, D), BF), pltpu.VMEM((D, D), BF),
            pltpu.VMEM((D, D), BF), pltpu.VMEM((D, D), BF),
            pltpu.VMEM((CHIPS, 4, BLK, 128), BF),
            pltpu.VMEM((NBLK + 2, BLK, 128), BF),
            pltpu.VMEM((CHIPS, QROWS, 128), BF),
            pltpu.VMEM((CHIPS, QROWS, 128), BF),
            pltpu.VMEM((CHIPS, 8, 16, 128), BF),
            pltpu.VMEM((CHIPS, 8, 16, 128), BF),
            pltpu.VMEM((16, 128), BF),
            pltpu.VMEM((SHARDS, 16, 128), BF),
            pltpu.VMEM((CHIPS, RAND, 4, HEADS), jnp.int32),
            pltpu.SMEM((CHIPS, RAND, 4, HEADS), jnp.int32),
            pltpu.VMEM((CHIPS * 4, BLK, 256), jnp.int32),
            pltpu.VMEM((4 * STEP, BLK, KEYS), F32),
            pltpu.VMEM((4 * STEP, BLK, KEYS), BF),
            pltpu.VMEM((4 * STEP, BLK, 128), F32),
            pltpu.VMEM((ROWS, 256), BF),
            pltpu.VMEM((ROWS, D), F32),
            dma((11,)), dma((9,)), dma, dma, dma, dma((CHIPS,)), dma, dma,
            dma, dma((GROUPS,)), dma, dma((GROUPS,)), dma, dma,
        ],
        compiler_params=pltpu.CompilerParams(
            collective_id=0, has_side_effects=True, vmem_limit_bytes=32 << 20
        ),
    )(*[
        pltpu.with_memory_space_constraint(x, pltpu.HBM)
        for x in (
            ids, lengths, tokens, norm_gain.reshape(1, D), norm_bias.reshape(1, D),
            pool_bias.reshape(1, D), w_query, w_key, w_value, w_out, w_pool,
        )
    ])


def solution(mesh):
    rows = P(("dp", "ctx"), None)
    placed = (
        rows, P(), P(), P(), P(), P(), P(), P(), P(),
        P(("dp", "ctx"), None, None), P("dp"),
    )
    return jax.shard_map(
        per_device,
        mesh=mesh,
        in_specs=placed,
        out_specs=(rows, P("dp", None)),
        check_vma=False,
    )
```

```python
import jax
import jax.numpy as jnp
from jax import lax
from jax.experimental import pallas as pl
from jax.experimental.pallas import tpu as pltpu
from jax.sharding import PartitionSpec as P

HEADS = 16
BLK = 64
RAND = 3
DOCS = 8
D = 1024
ROWS = 256
SEQ = 8192
NBLK = 128
SIDE = 4
CHIPS = 16
SHARDS = 32
QROWS = 136
KEYS = 6 * BLK

MESH = pl.DeviceIdType.MESH
BF = jnp.bfloat16
F32 = jnp.float32
MASKED = -240000.0
EXP_SCALE = 0.125 * 1.4426950408889634


ORDER_X = (3, 2, 1, 0)
ORDER_Z = (0, 1, 3, 2)
OWN = 12
STEP = 4
GROUPS = CHIPS // STEP


def kernel(
    ids_hbm, len_hbm, tok_hbm, gain_hbm, bias_hbm, pbias_hbm,
    wq_hbm, wk_hbm, wv_hbm, wo_hbm, wp_hbm,
    enc_ref, doc_ref,
    ids_ref, len_ref, tok_ref, gain_ref, bias_ref, pbias_ref, wq, wk, wv, wo, wp,
    kv_send, kv_buf, q_send, q_recv, att_send, att_recv, doc_send, doc_near, doc_sum, doc_recv,
    ids_row, ids_recv, ids_smem, masks, scores, weights, inverse, lhs, mixed,
    w_sem, own_sem, ids_ss, ids_rs, kv_ss, kv_rs, sib_ss, sib_rs,
    q_ss, q_rs, att_ss, att_rs, near_ss, near_rs, doc_ss, doc_rs,
):
    dp = lax.axis_index("dp")
    me = lax.axis_index("ctx")
    core = lax.rem(me, 2)
    chip = lax.div(me, 2)
    cx = lax.div(chip, SIDE)
    cz = lax.rem(chip, SIDE)

    ahead_x = [lax.rem(cx + d, SIDE) for d in ORDER_X]
    ahead_z = [lax.rem(cz + d, SIDE) for d in ORDER_Z]
    back_x = [lax.rem(cx + SIDE - d, SIDE) for d in ORDER_X]
    back_z = [lax.rem(cz + SIDE - d, SIDE) for d in ORDER_Z]
    others = [k for k in range(CHIPS) if k != OWN]
    ahead = [x * SIDE + z for x in ahead_x for z in ahead_z]
    back = [x * SIDE + z for x in back_x for z in back_z]

    def to_ctx(c):
        return (dp, 2 * c + core)

    sibling = (dp, 2 * chip + 1 - core)

    barrier = pltpu.get_barrier_semaphore()

    def greet(device):
        pl.semaphore_signal(barrier, inc=1, device_id=device, device_id_type=MESH)

    def tok_load():
        return pltpu.make_async_copy(tok_hbm, tok_ref, own_sem.at[0])

    def kv_load(g, n):
        cols = pl.ds(pl.multiple_of(g * 256, 256), 256)
        src, dst = ((wk_hbm, wk), (wv_hbm, wv))[n]
        return pltpu.make_async_copy(src.at[:, cols], dst.at[:, cols], w_sem.at[2 * g + n])

    def late_load(n):
        src, dst = ((wq_hbm, wq), (wo_hbm, wo), (wp_hbm, wp))[n]
        return pltpu.make_async_copy(src, dst, w_sem.at[8 + n])

    def small_load(n):
        src, dst = (
            (len_hbm, len_ref), (ids_hbm, ids_ref), (gain_hbm, gain_ref),
            (bias_hbm, bias_ref), (pbias_hbm, pbias_ref),
        )[n]
        return pltpu.make_async_copy(src, dst, own_sem.at[4 + n])

    for k in others:
        greet(to_ctx(ahead[k]))
    greet(sibling)
    tok_load().start()
    for g in range(4):
        for n in range(2):
            kv_load(g, n).start()
    for n in range(5):
        small_load(n).start()
    for n in range(3):
        late_load(n).start()

    lane = lax.broadcasted_iota(jnp.int32, (1, 128), 1)
    low = lane < 64

    def interleave(first, second):
        return (
            jnp.where(low, first, pltpu.roll(second, 64, 1)),
            jnp.where(low, pltpu.roll(first, 64, 1), second),
        )

    def rows_of(i):
        return pl.ds(4 * i + 1, 4)

    tok_load().wait()

    def kv_step(g, carry):
        kv_load(g, 0).wait()
        kv_load(g, 1).wait()
        cols = pl.ds(pl.multiple_of(g * 256, 256), 256)
        k = jnp.dot(tok_ref[...], wk[:, cols], preferred_element_type=F32)
        v = jnp.dot(tok_ref[...], wv[:, cols], preferred_element_type=F32)
        for p in range(2):
            s = slice(128 * p, 128 * p + 128)
            even, odd = interleave(k[:, s], v[:, s])
            kv_send[4 * g + 2 * p] = even.astype(BF).reshape(4, BLK, 128)
            kv_send[4 * g + 2 * p + 1] = odd.astype(BF).reshape(4, BLK, 128)
        return carry

    lax.fori_loop(0, 4, kv_step, 0)

    small_load(1).wait()
    row_ids = [ids_ref[r, b:b + 1, :] for r in range(RAND) for b in range(4)]
    ids_row[:, 0:128] = jnp.concatenate(row_ids[:8], axis=1)
    ids_row[:, 128:256] = jnp.concatenate(row_ids[8:] + row_ids[8:], axis=1)

    pl.semaphore_wait(barrier, CHIPS)

    def remote(src, dst, send_sem, recv_sem, device):
        return pltpu.make_async_remote_copy(
            src_ref=src, dst_ref=dst, send_sem=send_sem, recv_sem=recv_sem,
            device_id=device, device_id_type=MESH,
        )

    def ids_copy(k):
        return remote(ids_row, ids_recv.at[chip], ids_ss, ids_rs, to_ctx(ahead[k]))

    def kv_copy(k):
        return remote(
            kv_send.at[ahead[k]], kv_buf.at[rows_of(me)], kv_ss, kv_rs.at[k], to_ctx(ahead[k])
        )

    def q_copy(k):
        return remote(
            q_send.at[ahead[k]], q_recv.at[k], q_ss, q_rs.at[k // STEP], to_ctx(ahead[k])
        )

    def sib_copy(k):
        rows = rows_of(2 * back[k] + core)
        src = kv_send.at[chip] if k == OWN else kv_buf.at[rows]
        return remote(src, kv_buf.at[rows], sib_ss, sib_rs, sibling)

    def doc_copy(j):
        return remote(doc_sum, doc_recv.at[chip], doc_ss, doc_rs, to_ctx(ahead[j]))

    def drain(ref, sem):
        pltpu.make_async_copy(ref, ref, sem).wait()

    for k in others:
        ids_copy(k).start()
    for k in others:
        kv_copy(k).start()
    pltpu.make_async_copy(ids_row, ids_recv.at[chip], ids_rs).start()
    sib_copy(OWN).start()
    pltpu.make_async_copy(kv_send.at[chip], kv_buf.at[rows_of(me)], own_sem.at[1]).start()

    small_load(0).wait()
    ends, starts = [], []
    total = jnp.int32(0)
    for d in range(DOCS):
        starts.append(total)
        total = total + len_ref[d]
        ends.append(total)

    first_row = me * ROWS
    pick_row = lax.broadcasted_iota(jnp.int32, (8, 1), 0)
    pick = jnp.full((8, 1), -1, jnp.int32)
    for d in range(DOCS):
        pick = jnp.where(pick_row == d, starts[d], pick)
    pos = first_row + lax.broadcasted_iota(jnp.int32, (1, ROWS), 1)
    chooser = jnp.where(pick == pos, 1.0, 0.0).astype(BF)

    late_load(0).wait()

    def q_step(g, carry):
        cols = pl.ds(pl.multiple_of(g * 256, 256), 256)
        q = jnp.dot(tok_ref[...], wq[:, cols], preferred_element_type=F32)
        t = jnp.dot(chooser, tok_ref[:, cols], preferred_element_type=F32)
        for p in range(2):
            s = slice(128 * p, 128 * p + 128)
            even, odd = interleave(q[:128, s], q[128:, s])
            q_send[4 * g + 2 * p, 0:128, :] = even.astype(BF)
            q_send[4 * g + 2 * p + 1, 0:128, :] = odd.astype(BF)
            q_send[4 * g + 2 * p, 128:QROWS, :] = t[:, s].astype(BF)
            q_send[4 * g + 2 * p + 1, 128:QROWS, :] = pltpu.roll(t[:, s], 64, 1).astype(BF)
        return carry

    lax.fori_loop(0, 4, q_step, 0)
    for k in others:
        q_copy(k).start()
    pltpu.make_async_copy(q_send.at[chip], q_recv.at[OWN], q_rs.at[OWN // STEP]).start()

    kv_buf[0] = jnp.zeros((BLK, 128), BF)
    kv_buf[NBLK + 1] = jnp.zeros((BLK, 128), BF)

    col = lax.broadcasted_iota(jnp.int32, (1, 256), 1)
    diagonal = (
        lax.broadcasted_iota(jnp.int32, (BLK, 128), 1)
        == lax.broadcasted_iota(jnp.int32, (BLK, 128), 0) + BLK
    )

    def make_masks(k):
        first = (2 * back[k] + core) * (ROWS // BLK)
        for block in range(4):
            kpos = (first + block - 1) * BLK + col
            kdoc = jnp.zeros((1, 256), F32)
            for d in range(DOCS):
                kdoc = kdoc + jnp.where(kpos >= ends[d], 1.0, 0.0)
            kdoc = jnp.where((kpos < 0) | (kpos >= SEQ), -1.0, kdoc)
            qdoc = jnp.sum(jnp.where(diagonal, kdoc[:, :128], 0.0), axis=1, keepdims=True)
            keep = (qdoc == kdoc) | (col >= 3 * BLK)
            masks[4 * k + block] = jnp.where(keep, 1, 0)

    drain(ids_recv, ids_rs)
    to_smem = pltpu.make_async_copy(ids_recv, ids_smem, own_sem.at[3])
    to_smem.start()
    make_masks(OWN)
    for k in others:
        make_masks(k)
        kv_copy(k).wait_recv()
        sib_copy(k).start()
    to_smem.wait()
    drain(kv_send.at[0], own_sem.at[1])
    drain(kv_send, sib_rs)

    def attend(g, carry):
        drain(q_recv.at[pl.ds(0, STEP)], q_rs.at[g])
        homes = []
        for i in range(STEP):
            x = lax.rem(cx + 1 + g, SIDE)
            homes.append(x * SIDE + back_z[i])

        def keys_of(i, block):
            c = homes[i]
            b = (2 * c + core) * (ROWS // BLK) + block
            parts = [kv_buf[pl.ds(b, 3)].reshape(3 * BLK, 128)]
            for r in range(RAND):
                at = ids_smem[c, 0, (4 * r + block) * HEADS + chip]
                parts.append(kv_buf[at + 1])
            return jnp.concatenate(parts, axis=0)

        def score(i):
            for j in range(2):
                pair = q_recv[g * STEP + i, BLK * j:BLK * j + BLK, :].astype(F32)
                for half in range(2):
                    block = j + 2 * half
                    q = pltpu.roll(pair, 64, 1) if half else pair
                    q = jnp.where(low, q, 0.0).astype(BF)
                    scores[4 * i + block] = lax.dot_general(
                        q, keys_of(i, block), (((1,), (1,)), ((), ())),
                        preferred_element_type=F32,
                    )

        def soften(i):
            for block in range(4):
                t = 4 * i + block
                keep = masks[4 * (g * STEP + i) + block] > 0
                s0 = jnp.where(keep, scores[t, :, 0:256], MASKED)
                s1 = scores[t, :, 256:KEYS]
                m = jnp.maximum(jnp.maximum(s0[:, :128], s0[:, 128:]), s1)
                m = jnp.max(m, axis=1, keepdims=True)
                w0 = jnp.exp2((s0 - m) * EXP_SCALE)
                w1 = jnp.exp2((s1 - m) * EXP_SCALE)
                weights[t, :, 0:256] = w0.astype(BF)
                weights[t, :, 256:KEYS] = w1.astype(BF)
                l = jnp.sum(w0[:, :128] + w0[:, 128:] + w1, axis=1, keepdims=True)
                inverse[t] = jnp.broadcast_to(1.0 / l, (BLK, 128))

        def gather(i):
            for j in range(2):
                outs = []
                for half in range(2):
                    t = 4 * i + j + 2 * half
                    o = jnp.dot(
                        weights[t], keys_of(i, j + 2 * half), preferred_element_type=F32
                    )
                    outs.append(o * inverse[t])
                att_send[homes[i], 4 * j:4 * j + 4] = jnp.where(
                    low, pltpu.roll(outs[0], 64, 1), outs[1]
                ).astype(BF).reshape(4, 16, 128)

        def give_back(i):
            def send():
                remote(
                    att_send.at[homes[i]], att_recv.at[chip], att_ss, att_rs.at[g],
                    to_ctx(homes[i]),
                ).start()

            if i == OWN % STEP:
                pl.when(g != OWN // STEP)(send)
            else:
                send()

        for i in range(STEP):
            score(i)
        for i in range(STEP):
            soften(i)
        for i in range(STEP):
            gather(i)
        for i in range(STEP):
            give_back(i)

        return carry

    lax.fori_loop(0, GROUPS, attend, 0)
    pltpu.make_async_copy(att_send.at[chip], att_recv.at[chip], att_rs.at[GROUPS - 1]).start()

    tok_piece = jnp.zeros((8, 128), F32)
    for k in range(CHIPS):
        tok_piece = tok_piece + q_recv[k, 128:QROWS, :].astype(F32)
    att_piece = jnp.zeros((8, 128), F32)
    row8 = lax.broadcasted_iota(jnp.int32, (8, 1), 0)
    row16 = lax.broadcasted_iota(jnp.int32, (16, 1), 0)
    for d in range(DOCS):
        home = lax.div(starts[d], ROWS)
        local = lax.rem(starts[d], ROWS)
        packed = lax.rem(local, 128)
        tile = att_send[lax.div(home, 2), lax.div(packed, 16)].astype(F32)
        here = row16 + 16 * core == lax.rem(packed, 16) + 16 * lax.rem(home, 2)
        one = jnp.where(here, tile, 0.0)
        one = jnp.sum(one, axis=0, keepdims=True)
        one = jnp.where(lane * 0 + local >= 128, pltpu.roll(one, 64, 1), one)
        att_piece = jnp.where(row8 == d, one, att_piece)
    doc_send[...] = jnp.concatenate((att_piece, tok_piece), axis=0).astype(BF)
    near = remote(doc_send, doc_near, near_ss, near_rs, sibling)
    near.start()

    for n in range(2, 5):
        small_load(n).wait()

    def normed(rows):
        centre = jnp.mean(rows, axis=1, keepdims=True)
        spread = jnp.mean(jnp.square(rows - centre), axis=1, keepdims=True)
        return ((rows - centre) * lax.rsqrt(spread + 1e-05) * gain_ref[...] + bias_ref[...]).astype(BF)

    late_load(2).wait()
    def documents():
        drain(doc_recv, doc_rs)
        pieces = [doc_recv[h].astype(F32) for h in range(CHIPS)]
        opened = jnp.concatenate(
            [
                jnp.where(low, pieces[2 * j], pltpu.roll(pieces[2 * j + 1], 64, 1))
                for j in range(CHIPS // 2)
            ],
            axis=1,
        )
        y = jnp.dot(opened.astype(BF), wo[...], preferred_element_type=F32)
        doc_ref[...] = jnp.tanh(
            jnp.dot(normed(opened[8:] + y[:8]), wp[...], preferred_element_type=F32)
            + pbias_ref[...]
        )


    late_load(1).wait()
    for g in range(4):
        if g == 3:
            documents()
        drain(att_recv.at[pl.ds(0, 4)], att_rs.at[g])
        x = ahead_x[g]
        for p in range(2):
            even = att_recv[4 * x + 2 * p].reshape(128, 128).astype(F32)
            odd = att_recv[4 * x + 2 * p + 1].reshape(128, 128).astype(F32)
            top, bottom = interleave(even, odd)
            s = slice(128 * p, 128 * p + 128)
            lhs[0:128, s] = top.astype(BF)
            lhs[128:256, s] = bottom.astype(BF)
        heads = pl.ds(pl.multiple_of(x * 256, 256), 256)
        y = jnp.dot(lhs[...], wo[heads, :], preferred_element_type=F32)
        if g == 0:
            mixed[...] = tok_ref[...].astype(F32) + y
        else:
            mixed[...] = mixed[...] + y
        if g == 0:
            near.wait_recv()
            doc_sum[...] = (doc_send[...].astype(F32) + doc_near[...].astype(F32)).astype(BF)
            for k in others:
                doc_copy(k).start()
            pltpu.make_async_copy(doc_sum, doc_recv.at[chip], doc_rs).start()

    for n in range(8):
        rows = slice(32 * n, 32 * n + 32)
        enc_ref[rows, :] = normed(mixed[rows, :])

    most = pl.ds(0, CHIPS - 1)
    drain(ids_recv.at[most], ids_ss)
    drain(kv_send.at[most], kv_ss)
    drain(q_send.at[most], q_ss)
    drain(att_send.at[most], att_ss)
    drain(kv_send, sib_ss)
    near.wait_send()
    drain(doc_recv.at[most], doc_ss)


def per_device(
    tokens, w_query, w_key, w_value, w_out, norm_gain, norm_bias, w_pool, pool_bias,
    random_ids, lengths,
):
    vmem = pl.BlockSpec(memory_space=pltpu.VMEM)
    hbm = pl.BlockSpec(memory_space=pltpu.HBM)
    ids = random_ids.transpose(2, 0, 1)
    dma = pltpu.SemaphoreType.DMA
    return pl.pallas_call(
        kernel,
        out_shape=(
            jax.ShapeDtypeStruct((ROWS, D), BF),
            jax.ShapeDtypeStruct((DOCS, D), F32),
        ),
        in_specs=[hbm] * 11,
        out_specs=(vmem, vmem),
        scratch_shapes=[
            pltpu.VMEM((RAND, 4, HEADS), jnp.int32), pltpu.SMEM((DOCS,), jnp.int32),
            pltpu.VMEM((ROWS, D), BF),
            pltpu.VMEM((1, D), F32), pltpu.VMEM((1, D), F32), pltpu.VMEM((1, D), F32),
            pltpu.VMEM((D, D), BF), pltpu.VMEM((D, D), BF), pltpu.VMEM((D, D), BF),
            pltpu.VMEM((D, D), BF), pltpu.VMEM((D, D), BF),
            pltpu.VMEM((CHIPS, 4, BLK, 128), BF),
            pltpu.VMEM((NBLK + 2, BLK, 128), BF),
            pltpu.VMEM((CHIPS, QROWS, 128), BF),
            pltpu.VMEM((CHIPS, QROWS, 128), BF),
            pltpu.VMEM((CHIPS, 8, 16, 128), BF),
            pltpu.VMEM((CHIPS, 8, 16, 128), BF),
            pltpu.VMEM((16, 128), BF), pltpu.VMEM((16, 128), BF), pltpu.VMEM((16, 128), BF),
            pltpu.VMEM((CHIPS, 16, 128), BF),
            pltpu.VMEM((1, 256), jnp.int32),
            pltpu.VMEM((CHIPS, 1, 256), jnp.int32),
            pltpu.SMEM((CHIPS, 1, 256), jnp.int32),
            pltpu.VMEM((CHIPS * 4, BLK, 256), jnp.int32),
            pltpu.VMEM((4 * STEP, BLK, KEYS), F32),
            pltpu.VMEM((4 * STEP, BLK, KEYS), BF),
            pltpu.VMEM((4 * STEP, BLK, 128), F32),
            pltpu.VMEM((ROWS, 256), BF),
            pltpu.VMEM((ROWS, D), F32),
            dma((11,)), dma((9,)), dma, dma, dma, dma((CHIPS,)), dma, dma,
            dma, dma((GROUPS,)), dma, dma((GROUPS,)), dma, dma, dma, dma,
        ],
        compiler_params=pltpu.CompilerParams(
            collective_id=0, has_side_effects=True, vmem_limit_bytes=32 << 20
        ),
    )(*[
        pltpu.with_memory_space_constraint(x, pltpu.HBM)
        for x in (
            ids, lengths, tokens, norm_gain.reshape(1, D), norm_bias.reshape(1, D),
            pool_bias.reshape(1, D), w_query, w_key, w_value, w_out, w_pool,
        )
    ])


def solution(mesh):
    rows = P(("dp", "ctx"), None)
    placed = (
        rows, P(), P(), P(), P(), P(), P(), P(), P(),
        P(("dp", "ctx"), None, None), P("dp"),
    )
    return jax.shard_map(
        per_device,
        mesh=mesh,
        in_specs=placed,
        out_specs=(rows, P("dp", None)),
        check_vma=False,
    )
```

```python
import jax
import jax.numpy as jnp
from jax import lax
from jax.experimental import pallas as pl
from jax.experimental.pallas import tpu as pltpu
from jax.sharding import PartitionSpec as P

HEADS = 16
BLK = 64
RAND = 3
DOCS = 8
D = 1024
ROWS = 256
SEQ = 8192
NBLK = 128
SIDE = 4
CHIPS = 16
SHARDS = 32
QROWS = 136
KEYS = 6 * BLK

MESH = pl.DeviceIdType.MESH
BF = jnp.bfloat16
F32 = jnp.float32
MASKED = -240000.0
EXP_SCALE = 0.125 * 1.4426950408889634


ORDER_X = (3, 2, 1, 0)
ORDER_Z = (0, 1, 3, 2)
OWN = 12
KV_STEPS = (
    (1, 0), (3, 0), (0, 2), (1, 2), (3, 2), (0, 1), (0, 3), (1, 1),
    (3, 3), (2, 2), (1, 3), (3, 1), (2, 0), (2, 1), (2, 3),
)
KV_ORDER = [SIDE * ORDER_X.index(dx) + ORDER_Z.index(dz) for dx, dz in KV_STEPS]
STEP = 4
GROUPS = CHIPS // STEP


def kernel(
    ids_hbm, len_hbm, tok_hbm, gain_hbm, bias_hbm, pbias_hbm,
    wq_hbm, wk_hbm, wv_hbm, wo_hbm, wp_hbm,
    enc_ref, doc_ref,
    ids_ref, len_ref, tok_ref, gain_ref, bias_ref, pbias_ref, wq, wk, wv, wo, wp,
    kv_send, kv_buf, q_send, q_recv, att_send, att_recv, doc_send, doc_near, doc_sum, doc_recv,
    ids_row, ids_recv, ids_smem, masks, scores, weights, inverse, lhs, mixed,
    w_sem, own_sem, ids_ss, ids_rs, kv_ss, kv_rs, sib_ss, sib_rs,
    q_ss, q_rs, att_ss, att_rs, near_ss, near_rs, doc_ss, doc_rs,
):
    dp = lax.axis_index("dp")
    me = lax.axis_index("ctx")
    core = lax.rem(me, 2)
    chip = lax.div(me, 2)
    cx = lax.div(chip, SIDE)
    cz = lax.rem(chip, SIDE)

    ahead_x = [lax.rem(cx + d, SIDE) for d in ORDER_X]
    ahead_z = [lax.rem(cz + d, SIDE) for d in ORDER_Z]
    back_x = [lax.rem(cx + SIDE - d, SIDE) for d in ORDER_X]
    back_z = [lax.rem(cz + SIDE - d, SIDE) for d in ORDER_Z]
    others = [k for k in range(CHIPS) if k != OWN]
    ahead = [x * SIDE + z for x in ahead_x for z in ahead_z]
    back = [x * SIDE + z for x in back_x for z in back_z]

    def to_ctx(c):
        return (dp, 2 * c + core)

    sibling = (dp, 2 * chip + 1 - core)

    barrier = pltpu.get_barrier_semaphore()

    def greet(device):
        pl.semaphore_signal(barrier, inc=1, device_id=device, device_id_type=MESH)

    def tok_load():
        return pltpu.make_async_copy(tok_hbm, tok_ref, own_sem.at[0])

    def kv_load(g, n):
        cols = pl.ds(pl.multiple_of(g * 256, 256), 256)
        src, dst = ((wk_hbm, wk), (wv_hbm, wv))[n]
        return pltpu.make_async_copy(src.at[:, cols], dst.at[:, cols], w_sem.at[2 * g + n])

    def late_load(n):
        src, dst = ((wq_hbm, wq), (wo_hbm, wo), (wp_hbm, wp))[n]
        return pltpu.make_async_copy(src, dst, w_sem.at[8 + n])

    def small_load(n):
        src, dst = (
            (len_hbm, len_ref), (ids_hbm, ids_ref), (gain_hbm, gain_ref),
            (bias_hbm, bias_ref), (pbias_hbm, pbias_ref),
        )[n]
        return pltpu.make_async_copy(src, dst, own_sem.at[4 + n])

    for k in others:
        greet(to_ctx(ahead[k]))
    greet(sibling)
    tok_load().start()
    for g in range(4):
        for n in range(2):
            kv_load(g, n).start()
    for n in range(5):
        small_load(n).start()
    for n in range(3):
        late_load(n).start()

    lane = lax.broadcasted_iota(jnp.int32, (1, 128), 1)
    low = lane < 64

    def interleave(first, second):
        return (
            jnp.where(low, first, pltpu.roll(second, 64, 1)),
            jnp.where(low, pltpu.roll(first, 64, 1), second),
        )

    def rows_of(i):
        return pl.ds(4 * i + 1, 4)

    tok_load().wait()

    def kv_step(g, carry):
        kv_load(g, 0).wait()
        kv_load(g, 1).wait()
        cols = pl.ds(pl.multiple_of(g * 256, 256), 256)
        k = jnp.dot(tok_ref[...], wk[:, cols], preferred_element_type=F32)
        v = jnp.dot(tok_ref[...], wv[:, cols], preferred_element_type=F32)
        for p in range(2):
            s = slice(128 * p, 128 * p + 128)
            even, odd = interleave(k[:, s], v[:, s])
            kv_send[4 * g + 2 * p] = even.astype(BF).reshape(4, BLK, 128)
            kv_send[4 * g + 2 * p + 1] = odd.astype(BF).reshape(4, BLK, 128)
        return carry

    lax.fori_loop(0, 4, kv_step, 0)

    small_load(1).wait()
    row_ids = [ids_ref[r, b:b + 1, :] for r in range(RAND) for b in range(4)]
    ids_row[:, 0:128] = jnp.concatenate(row_ids[:8], axis=1)
    ids_row[:, 128:256] = jnp.concatenate(row_ids[8:] + row_ids[8:], axis=1)

    pl.semaphore_wait(barrier, CHIPS)

    def remote(src, dst, send_sem, recv_sem, device):
        return pltpu.make_async_remote_copy(
            src_ref=src, dst_ref=dst, send_sem=send_sem, recv_sem=recv_sem,
            device_id=device, device_id_type=MESH,
        )

    def ids_copy(k):
        return remote(ids_row, ids_recv.at[chip], ids_ss, ids_rs, to_ctx(ahead[k]))

    def kv_copy(k):
        return remote(
            kv_send.at[ahead[k]], kv_buf.at[rows_of(me)], kv_ss, kv_rs.at[k], to_ctx(ahead[k])
        )

    def q_copy(k):
        return remote(
            q_send.at[ahead[k]], q_recv.at[k], q_ss, q_rs.at[k // STEP], to_ctx(ahead[k])
        )

    def sib_copy(k):
        rows = rows_of(2 * back[k] + core)
        src = kv_send.at[chip] if k == OWN else kv_buf.at[rows]
        return remote(src, kv_buf.at[rows], sib_ss, sib_rs, sibling)

    def doc_copy(j):
        return remote(doc_sum, doc_recv.at[chip], doc_ss, doc_rs, to_ctx(ahead[j]))

    def drain(ref, sem):
        pltpu.make_async_copy(ref, ref, sem).wait()

    for k in others:
        ids_copy(k).start()
    for k in KV_ORDER:
        kv_copy(k).start()
    pltpu.make_async_copy(ids_row, ids_recv.at[chip], ids_rs).start()
    sib_copy(OWN).start()
    pltpu.make_async_copy(kv_send.at[chip], kv_buf.at[rows_of(me)], own_sem.at[1]).start()

    small_load(0).wait()
    ends, starts = [], []
    total = jnp.int32(0)
    for d in range(DOCS):
        starts.append(total)
        total = total + len_ref[d]
        ends.append(total)

    first_row = me * ROWS
    pick_row = lax.broadcasted_iota(jnp.int32, (8, 1), 0)
    pick = jnp.full((8, 1), -1, jnp.int32)
    for d in range(DOCS):
        pick = jnp.where(pick_row == d, starts[d], pick)
    pos = first_row + lax.broadcasted_iota(jnp.int32, (1, ROWS), 1)
    chooser = jnp.where(pick == pos, 1.0, 0.0).astype(BF)

    late_load(0).wait()

    def q_step(g, carry):
        cols = pl.ds(pl.multiple_of(g * 256, 256), 256)
        q = jnp.dot(tok_ref[...], wq[:, cols], preferred_element_type=F32)
        t = jnp.dot(chooser, tok_ref[:, cols], preferred_element_type=F32)
        for p in range(2):
            s = slice(128 * p, 128 * p + 128)
            even, odd = interleave(q[:128, s], q[128:, s])
            q_send[4 * g + 2 * p, 0:128, :] = even.astype(BF)
            q_send[4 * g + 2 * p + 1, 0:128, :] = odd.astype(BF)
            q_send[4 * g + 2 * p, 128:QROWS, :] = t[:, s].astype(BF)
            q_send[4 * g + 2 * p + 1, 128:QROWS, :] = pltpu.roll(t[:, s], 64, 1).astype(BF)
        return carry

    lax.fori_loop(0, 4, q_step, 0)
    for k in others:
        q_copy(k).start()
    pltpu.make_async_copy(q_send.at[chip], q_recv.at[OWN], q_rs.at[OWN // STEP]).start()

    kv_buf[0] = jnp.zeros((BLK, 128), BF)
    kv_buf[NBLK + 1] = jnp.zeros((BLK, 128), BF)

    col = lax.broadcasted_iota(jnp.int32, (1, 256), 1)
    diagonal = (
        lax.broadcasted_iota(jnp.int32, (BLK, 128), 1)
        == lax.broadcasted_iota(jnp.int32, (BLK, 128), 0) + BLK
    )

    def make_masks(k):
        first = (2 * back[k] + core) * (ROWS // BLK)
        for block in range(4):
            kpos = (first + block - 1) * BLK + col
            kdoc = jnp.zeros((1, 256), F32)
            for d in range(DOCS):
                kdoc = kdoc + jnp.where(kpos >= ends[d], 1.0, 0.0)
            kdoc = jnp.where((kpos < 0) | (kpos >= SEQ), -1.0, kdoc)
            qdoc = jnp.sum(jnp.where(diagonal, kdoc[:, :128], 0.0), axis=1, keepdims=True)
            keep = (qdoc == kdoc) | (col >= 3 * BLK)
            masks[4 * k + block] = jnp.where(keep, 1, 0)

    drain(ids_recv, ids_rs)
    to_smem = pltpu.make_async_copy(ids_recv, ids_smem, own_sem.at[3])
    to_smem.start()
    make_masks(OWN)
    for k in KV_ORDER:
        make_masks(k)
        kv_copy(k).wait_recv()
        sib_copy(k).start()
    to_smem.wait()
    drain(kv_send.at[0], own_sem.at[1])
    drain(kv_send, sib_rs)

    def attend(g, carry):
        drain(q_recv.at[pl.ds(0, STEP)], q_rs.at[g])
        homes = []
        for i in range(STEP):
            x = lax.rem(cx + 1 + g, SIDE)
            homes.append(x * SIDE + back_z[i])

        def keys_of(i, block):
            c = homes[i]
            b = (2 * c + core) * (ROWS // BLK) + block
            parts = [kv_buf[pl.ds(b, 3)].reshape(3 * BLK, 128)]
            for r in range(RAND):
                at = ids_smem[c, 0, (4 * r + block) * HEADS + chip]
                parts.append(kv_buf[at + 1])
            return jnp.concatenate(parts, axis=0)

        def score(i):
            for j in range(2):
                pair = q_recv[g * STEP + i, BLK * j:BLK * j + BLK, :].astype(F32)
                for half in range(2):
                    block = j + 2 * half
                    q = pltpu.roll(pair, 64, 1) if half else pair
                    q = jnp.where(low, q, 0.0).astype(BF)
                    scores[4 * i + block] = lax.dot_general(
                        q, keys_of(i, block), (((1,), (1,)), ((), ())),
                        preferred_element_type=F32,
                    )

        def soften(i):
            for block in range(4):
                t = 4 * i + block
                keep = masks[4 * (g * STEP + i) + block] > 0
                s0 = jnp.where(keep, scores[t, :, 0:256], MASKED)
                s1 = scores[t, :, 256:KEYS]
                m = jnp.maximum(jnp.maximum(s0[:, :128], s0[:, 128:]), s1)
                m = jnp.max(m, axis=1, keepdims=True)
                w0 = jnp.exp2((s0 - m) * EXP_SCALE)
                w1 = jnp.exp2((s1 - m) * EXP_SCALE)
                weights[t, :, 0:256] = w0.astype(BF)
                weights[t, :, 256:KEYS] = w1.astype(BF)
                l = jnp.sum(w0[:, :128] + w0[:, 128:] + w1, axis=1, keepdims=True)
                inverse[t] = jnp.broadcast_to(1.0 / l, (BLK, 128))

        def gather(i):
            for j in range(2):
                outs = []
                for half in range(2):
                    t = 4 * i + j + 2 * half
                    o = jnp.dot(
                        weights[t], keys_of(i, j + 2 * half), preferred_element_type=F32
                    )
                    outs.append(o * inverse[t])
                att_send[homes[i], 4 * j:4 * j + 4] = jnp.where(
                    low, pltpu.roll(outs[0], 64, 1), outs[1]
                ).astype(BF).reshape(4, 16, 128)

        def give_back(i):
            def send():
                remote(
                    att_send.at[homes[i]], att_recv.at[chip], att_ss, att_rs.at[g],
                    to_ctx(homes[i]),
                ).start()

            if i == OWN % STEP:
                pl.when(g != OWN // STEP)(send)
            else:
                send()

        for i in range(STEP):
            score(i)
        for i in range(STEP):
            soften(i)
        for i in range(STEP):
            gather(i)
        for i in range(STEP):
            give_back(i)

        return carry

    lax.fori_loop(0, GROUPS, attend, 0)
    pltpu.make_async_copy(att_send.at[chip], att_recv.at[chip], att_rs.at[GROUPS - 1]).start()

    tok_piece = jnp.zeros((8, 128), F32)
    for k in range(CHIPS):
        tok_piece = tok_piece + q_recv[k, 128:QROWS, :].astype(F32)
    att_piece = jnp.zeros((8, 128), F32)
    row8 = lax.broadcasted_iota(jnp.int32, (8, 1), 0)
    row16 = lax.broadcasted_iota(jnp.int32, (16, 1), 0)
    for d in range(DOCS):
        home = lax.div(starts[d], ROWS)
        local = lax.rem(starts[d], ROWS)
        packed = lax.rem(local, 128)
        tile = att_send[lax.div(home, 2), lax.div(packed, 16)].astype(F32)
        here = row16 + 16 * core == lax.rem(packed, 16) + 16 * lax.rem(home, 2)
        one = jnp.where(here, tile, 0.0)
        one = jnp.sum(one, axis=0, keepdims=True)
        one = jnp.where(lane * 0 + local >= 128, pltpu.roll(one, 64, 1), one)
        att_piece = jnp.where(row8 == d, one, att_piece)
    doc_send[...] = jnp.concatenate((att_piece, tok_piece), axis=0).astype(BF)
    near = remote(doc_send, doc_near, near_ss, near_rs, sibling)
    near.start()

    for n in range(2, 5):
        small_load(n).wait()

    def normed(rows):
        centre = jnp.mean(rows, axis=1, keepdims=True)
        spread = jnp.mean(jnp.square(rows - centre), axis=1, keepdims=True)
        return ((rows - centre) * lax.rsqrt(spread + 1e-05) * gain_ref[...] + bias_ref[...]).astype(BF)

    late_load(2).wait()
    def documents():
        drain(doc_recv, doc_rs)
        pieces = [doc_recv[h].astype(F32) for h in range(CHIPS)]
        opened = jnp.concatenate(
            [
                jnp.where(low, pieces[2 * j], pltpu.roll(pieces[2 * j + 1], 64, 1))
                for j in range(CHIPS // 2)
            ],
            axis=1,
        )
        y = jnp.dot(opened.astype(BF), wo[...], preferred_element_type=F32)
        doc_ref[...] = jnp.tanh(
            jnp.dot(normed(opened[8:] + y[:8]), wp[...], preferred_element_type=F32)
            + pbias_ref[...]
        )


    late_load(1).wait()
    for g in range(4):
        if g == 3:
            documents()
        drain(att_recv.at[pl.ds(0, 4)], att_rs.at[g])
        x = ahead_x[g]
        for p in range(2):
            even = att_recv[4 * x + 2 * p].reshape(128, 128).astype(F32)
            odd = att_recv[4 * x + 2 * p + 1].reshape(128, 128).astype(F32)
            top, bottom = interleave(even, odd)
            s = slice(128 * p, 128 * p + 128)
            lhs[0:128, s] = top.astype(BF)
            lhs[128:256, s] = bottom.astype(BF)
        heads = pl.ds(pl.multiple_of(x * 256, 256), 256)
        y = jnp.dot(lhs[...], wo[heads, :], preferred_element_type=F32)
        if g == 0:
            mixed[...] = tok_ref[...].astype(F32) + y
        else:
            mixed[...] = mixed[...] + y
        if g == 0:
            near.wait_recv()
            doc_sum[...] = (doc_send[...].astype(F32) + doc_near[...].astype(F32)).astype(BF)
            for k in others:
                doc_copy(k).start()
            pltpu.make_async_copy(doc_sum, doc_recv.at[chip], doc_rs).start()

    for n in range(8):
        rows = slice(32 * n, 32 * n + 32)
        enc_ref[rows, :] = normed(mixed[rows, :])

    most = pl.ds(0, CHIPS - 1)
    drain(ids_recv.at[most], ids_ss)
    drain(kv_send.at[most], kv_ss)
    drain(q_send.at[most], q_ss)
    drain(att_send.at[most], att_ss)
    drain(kv_send, sib_ss)
    near.wait_send()
    drain(doc_recv.at[most], doc_ss)


def per_device(
    tokens, w_query, w_key, w_value, w_out, norm_gain, norm_bias, w_pool, pool_bias,
    random_ids, lengths,
):
    vmem = pl.BlockSpec(memory_space=pltpu.VMEM)
    hbm = pl.BlockSpec(memory_space=pltpu.HBM)
    ids = random_ids.transpose(2, 0, 1)
    dma = pltpu.SemaphoreType.DMA
    return pl.pallas_call(
        kernel,
        out_shape=(
            jax.ShapeDtypeStruct((ROWS, D), BF),
            jax.ShapeDtypeStruct((DOCS, D), F32),
        ),
        in_specs=[hbm] * 11,
        out_specs=(vmem, vmem),
        scratch_shapes=[
            pltpu.VMEM((RAND, 4, HEADS), jnp.int32), pltpu.SMEM((DOCS,), jnp.int32),
            pltpu.VMEM((ROWS, D), BF),
            pltpu.VMEM((1, D), F32), pltpu.VMEM((1, D), F32), pltpu.VMEM((1, D), F32),
            pltpu.VMEM((D, D), BF), pltpu.VMEM((D, D), BF), pltpu.VMEM((D, D), BF),
            pltpu.VMEM((D, D), BF), pltpu.VMEM((D, D), BF),
            pltpu.VMEM((CHIPS, 4, BLK, 128), BF),
            pltpu.VMEM((NBLK + 2, BLK, 128), BF),
            pltpu.VMEM((CHIPS, QROWS, 128), BF),
            pltpu.VMEM((CHIPS, QROWS, 128), BF),
            pltpu.VMEM((CHIPS, 8, 16, 128), BF),
            pltpu.VMEM((CHIPS, 8, 16, 128), BF),
            pltpu.VMEM((16, 128), BF), pltpu.VMEM((16, 128), BF), pltpu.VMEM((16, 128), BF),
            pltpu.VMEM((CHIPS, 16, 128), BF),
            pltpu.VMEM((1, 256), jnp.int32),
            pltpu.VMEM((CHIPS, 1, 256), jnp.int32),
            pltpu.SMEM((CHIPS, 1, 256), jnp.int32),
            pltpu.VMEM((CHIPS * 4, BLK, 256), jnp.int32),
            pltpu.VMEM((4 * STEP, BLK, KEYS), F32),
            pltpu.VMEM((4 * STEP, BLK, KEYS), BF),
            pltpu.VMEM((4 * STEP, BLK, 128), F32),
            pltpu.VMEM((ROWS, 256), BF),
            pltpu.VMEM((ROWS, D), F32),
            dma((11,)), dma((9,)), dma, dma, dma, dma((CHIPS,)), dma, dma,
            dma, dma((GROUPS,)), dma, dma((GROUPS,)), dma, dma, dma, dma,
        ],
        compiler_params=pltpu.CompilerParams(
            collective_id=0, has_side_effects=True, vmem_limit_bytes=32 << 20
        ),
    )(*[
        pltpu.with_memory_space_constraint(x, pltpu.HBM)
        for x in (
            ids, lengths, tokens, norm_gain.reshape(1, D), norm_bias.reshape(1, D),
            pool_bias.reshape(1, D), w_query, w_key, w_value, w_out, w_pool,
        )
    ])


def solution(mesh):
    rows = P(("dp", "ctx"), None)
    placed = (
        rows, P(), P(), P(), P(), P(), P(), P(), P(),
        P(("dp", "ctx"), None, None), P("dp"),
    )
    return jax.shard_map(
        per_device,
        mesh=mesh,
        in_specs=placed,
        out_specs=(rows, P("dp", None)),
        check_vma=False,
    )
```

```python
import jax
import jax.numpy as jnp
from jax import lax
from jax.experimental import pallas as pl
from jax.experimental.pallas import tpu as pltpu
from jax.sharding import PartitionSpec as P

HEADS = 16
BLK = 64
RAND = 3
DOCS = 8
D = 1024
ROWS = 256
SEQ = 8192
NBLK = 128
SIDE = 4
CHIPS = 16
SHARDS = 32
QROWS = 136
KEYS = 6 * BLK

MESH = pl.DeviceIdType.MESH
BF = jnp.bfloat16
F32 = jnp.float32
MASKED = -240000.0
EXP_SCALE = 0.125 * 1.4426950408889634


ORDER_X = (3, 2, 1, 0)
ORDER_Z = (0, 1, 3, 2)
OWN = 12
KV_STEPS = (
    (1, 0), (3, 0), (0, 2), (1, 2), (3, 2), (0, 1), (0, 3), (1, 1),
    (3, 3), (2, 2), (1, 3), (3, 1), (2, 0), (2, 1), (2, 3),
)
Q_ORDER = (0, 8, 1, 9, 2, 10, 3, 11, 4, 5, 6, 7, 13, 14, 15)
KV_ORDER = [SIDE * ORDER_X.index(dx) + ORDER_Z.index(dz) for dx, dz in KV_STEPS]
STEP = 4
GROUPS = CHIPS // STEP


def kernel(
    ids_hbm, len_hbm, tok_hbm, gain_hbm, bias_hbm, pbias_hbm,
    wq_hbm, wk_hbm, wv_hbm, wo_hbm, wp_hbm,
    enc_ref, doc_ref,
    ids_ref, len_ref, tok_ref, gain_ref, bias_ref, pbias_ref, wq, wk, wv, wo, wp,
    kv_send, kv_buf, q_send, q_recv, att_send, att_recv, doc_send, doc_near, doc_sum, doc_recv,
    ids_row, ids_recv, ids_smem, masks, scores, weights, inverse, lhs, mixed,
    w_sem, own_sem, ids_ss, ids_rs, kv_ss, kv_rs, sib_ss, sib_rs,
    q_ss, q_rs, att_ss, att_rs, near_ss, near_rs, doc_ss, doc_rs,
):
    dp = lax.axis_index("dp")
    me = lax.axis_index("ctx")
    core = lax.rem(me, 2)
    chip = lax.div(me, 2)
    cx = lax.div(chip, SIDE)
    cz = lax.rem(chip, SIDE)

    ahead_x = [lax.rem(cx + d, SIDE) for d in ORDER_X]
    ahead_z = [lax.rem(cz + d, SIDE) for d in ORDER_Z]
    back_x = [lax.rem(cx + SIDE - d, SIDE) for d in ORDER_X]
    back_z = [lax.rem(cz + SIDE - d, SIDE) for d in ORDER_Z]
    others = [k for k in range(CHIPS) if k != OWN]
    ahead = [x * SIDE + z for x in ahead_x for z in ahead_z]
    back = [x * SIDE + z for x in back_x for z in back_z]

    def to_ctx(c):
        return (dp, 2 * c + core)

    sibling = (dp, 2 * chip + 1 - core)

    barrier = pltpu.get_barrier_semaphore()

    def greet(device):
        pl.semaphore_signal(barrier, inc=1, device_id=device, device_id_type=MESH)

    def tok_load():
        return pltpu.make_async_copy(tok_hbm, tok_ref, own_sem.at[0])

    def kv_load(g, n):
        cols = pl.ds(pl.multiple_of(g * 256, 256), 256)
        src, dst = ((wk_hbm, wk), (wv_hbm, wv))[n]
        return pltpu.make_async_copy(src.at[:, cols], dst.at[:, cols], w_sem.at[2 * g + n])

    def late_load(n):
        src, dst = ((wq_hbm, wq), (wo_hbm, wo), (wp_hbm, wp))[n]
        return pltpu.make_async_copy(src, dst, w_sem.at[8 + n])

    def small_load(n):
        src, dst = (
            (len_hbm, len_ref), (ids_hbm, ids_ref), (gain_hbm, gain_ref),
            (bias_hbm, bias_ref), (pbias_hbm, pbias_ref),
        )[n]
        return pltpu.make_async_copy(src, dst, own_sem.at[4 + n])

    for k in others:
        greet(to_ctx(ahead[k]))
    greet(sibling)
    tok_load().start()
    for g in range(4):
        for n in range(2):
            kv_load(g, n).start()
    for n in range(5):
        small_load(n).start()
    for n in range(3):
        late_load(n).start()

    lane = lax.broadcasted_iota(jnp.int32, (1, 128), 1)
    low = lane < 64

    def interleave(first, second):
        return (
            jnp.where(low, first, pltpu.roll(second, 64, 1)),
            jnp.where(low, pltpu.roll(first, 64, 1), second),
        )

    def rows_of(i):
        return pl.ds(4 * i + 1, 4)

    tok_load().wait()

    def kv_step(g, carry):
        kv_load(g, 0).wait()
        kv_load(g, 1).wait()
        cols = pl.ds(pl.multiple_of(g * 256, 256), 256)
        k = jnp.dot(tok_ref[...], wk[:, cols], preferred_element_type=F32)
        v = jnp.dot(tok_ref[...], wv[:, cols], preferred_element_type=F32)
        for p in range(2):
            s = slice(128 * p, 128 * p + 128)
            even, odd = interleave(k[:, s], v[:, s])
            kv_send[4 * g + 2 * p] = even.astype(BF).reshape(4, BLK, 128)
            kv_send[4 * g + 2 * p + 1] = odd.astype(BF).reshape(4, BLK, 128)
        return carry

    lax.fori_loop(0, 4, kv_step, 0)

    small_load(1).wait()
    row_ids = [ids_ref[r, b:b + 1, :] for r in range(RAND) for b in range(4)]
    ids_row[:, 0:128] = jnp.concatenate(row_ids[:8], axis=1)
    ids_row[:, 128:256] = jnp.concatenate(row_ids[8:] + row_ids[8:], axis=1)

    pl.semaphore_wait(barrier, CHIPS)

    def remote(src, dst, send_sem, recv_sem, device):
        return pltpu.make_async_remote_copy(
            src_ref=src, dst_ref=dst, send_sem=send_sem, recv_sem=recv_sem,
            device_id=device, device_id_type=MESH,
        )

    def ids_copy(k):
        return remote(ids_row, ids_recv.at[chip], ids_ss, ids_rs, to_ctx(ahead[k]))

    def kv_copy(k):
        return remote(
            kv_send.at[ahead[k]], kv_buf.at[rows_of(me)], kv_ss, kv_rs.at[k], to_ctx(ahead[k])
        )

    def q_copy(k):
        return remote(
            q_send.at[ahead[k]], q_recv.at[k], q_ss, q_rs.at[k // STEP], to_ctx(ahead[k])
        )

    def sib_copy(k):
        rows = rows_of(2 * back[k] + core)
        src = kv_send.at[chip] if k == OWN else kv_buf.at[rows]
        return remote(src, kv_buf.at[rows], sib_ss, sib_rs, sibling)

    def doc_copy(j):
        return remote(doc_sum, doc_recv.at[chip], doc_ss, doc_rs, to_ctx(ahead[j]))

    def drain(ref, sem):
        pltpu.make_async_copy(ref, ref, sem).wait()

    for k in others:
        ids_copy(k).start()
    for k in KV_ORDER:
        kv_copy(k).start()
    pltpu.make_async_copy(ids_row, ids_recv.at[chip], ids_rs).start()
    sib_copy(OWN).start()
    pltpu.make_async_copy(kv_send.at[chip], kv_buf.at[rows_of(me)], own_sem.at[1]).start()

    small_load(0).wait()
    ends, starts = [], []
    total = jnp.int32(0)
    for d in range(DOCS):
        starts.append(total)
        total = total + len_ref[d]
        ends.append(total)

    first_row = me * ROWS
    pick_row = lax.broadcasted_iota(jnp.int32, (8, 1), 0)
    pick = jnp.full((8, 1), -1, jnp.int32)
    for d in range(DOCS):
        pick = jnp.where(pick_row == d, starts[d], pick)
    pos = first_row + lax.broadcasted_iota(jnp.int32, (1, ROWS), 1)
    chooser = jnp.where(pick == pos, 1.0, 0.0).astype(BF)

    late_load(0).wait()

    def q_step(g, carry):
        cols = pl.ds(pl.multiple_of(g * 256, 256), 256)
        q = jnp.dot(tok_ref[...], wq[:, cols], preferred_element_type=F32)
        t = jnp.dot(chooser, tok_ref[:, cols], preferred_element_type=F32)
        for p in range(2):
            s = slice(128 * p, 128 * p + 128)
            even, odd = interleave(q[:128, s], q[128:, s])
            q_send[4 * g + 2 * p, 0:128, :] = even.astype(BF)
            q_send[4 * g + 2 * p + 1, 0:128, :] = odd.astype(BF)
            q_send[4 * g + 2 * p, 128:QROWS, :] = t[:, s].astype(BF)
            q_send[4 * g + 2 * p + 1, 128:QROWS, :] = pltpu.roll(t[:, s], 64, 1).astype(BF)
        return carry

    lax.fori_loop(0, 4, q_step, 0)
    for k in Q_ORDER:
        q_copy(k).start()
    pltpu.make_async_copy(q_send.at[chip], q_recv.at[OWN], q_rs.at[OWN // STEP]).start()

    kv_buf[0] = jnp.zeros((BLK, 128), BF)
    kv_buf[NBLK + 1] = jnp.zeros((BLK, 128), BF)

    col = lax.broadcasted_iota(jnp.int32, (1, 256), 1)
    diagonal = (
        lax.broadcasted_iota(jnp.int32, (BLK, 128), 1)
        == lax.broadcasted_iota(jnp.int32, (BLK, 128), 0) + BLK
    )

    def make_masks(k):
        first = (2 * back[k] + core) * (ROWS // BLK)
        for block in range(4):
            kpos = (first + block - 1) * BLK + col
            kdoc = jnp.zeros((1, 256), F32)
            for d in range(DOCS):
                kdoc = kdoc + jnp.where(kpos >= ends[d], 1.0, 0.0)
            kdoc = jnp.where((kpos < 0) | (kpos >= SEQ), -1.0, kdoc)
            qdoc = jnp.sum(jnp.where(diagonal, kdoc[:, :128], 0.0), axis=1, keepdims=True)
            keep = (qdoc == kdoc) | (col >= 3 * BLK)
            masks[4 * k + block] = jnp.where(keep, 1, 0)

    drain(ids_recv, ids_rs)
    to_smem = pltpu.make_async_copy(ids_recv, ids_smem, own_sem.at[3])
    to_smem.start()
    make_masks(OWN)
    for k in KV_ORDER:
        make_masks(k)
        kv_copy(k).wait_recv()
        sib_copy(k).start()
    to_smem.wait()
    drain(kv_send.at[0], own_sem.at[1])
    drain(kv_send, sib_rs)

    def attend(g, carry):
        drain(q_recv.at[pl.ds(0, STEP)], q_rs.at[g])
        homes = []
        for i in range(STEP):
            x = lax.rem(cx + 1 + g, SIDE)
            homes.append(x * SIDE + back_z[i])

        def keys_of(i, block):
            c = homes[i]
            b = (2 * c + core) * (ROWS // BLK) + block
            parts = [kv_buf[pl.ds(b, 3)].reshape(3 * BLK, 128)]
            for r in range(RAND):
                at = ids_smem[c, 0, (4 * r + block) * HEADS + chip]
                parts.append(kv_buf[at + 1])
            return jnp.concatenate(parts, axis=0)

        def score(i):
            for j in range(2):
                pair = q_recv[g * STEP + i, BLK * j:BLK * j + BLK, :].astype(F32)
                for half in range(2):
                    block = j + 2 * half
                    q = pltpu.roll(pair, 64, 1) if half else pair
                    q = jnp.where(low, q, 0.0).astype(BF)
                    scores[4 * i + block] = lax.dot_general(
                        q, keys_of(i, block), (((1,), (1,)), ((), ())),
                        preferred_element_type=F32,
                    )

        def soften(i):
            for block in range(4):
                t = 4 * i + block
                keep = masks[4 * (g * STEP + i) + block] > 0
                s0 = jnp.where(keep, scores[t, :, 0:256], MASKED)
                s1 = scores[t, :, 256:KEYS]
                m = jnp.maximum(jnp.maximum(s0[:, :128], s0[:, 128:]), s1)
                m = jnp.max(m, axis=1, keepdims=True)
                w0 = jnp.exp2((s0 - m) * EXP_SCALE)
                w1 = jnp.exp2((s1 - m) * EXP_SCALE)
                weights[t, :, 0:256] = w0.astype(BF)
                weights[t, :, 256:KEYS] = w1.astype(BF)
                l = jnp.sum(w0[:, :128] + w0[:, 128:] + w1, axis=1, keepdims=True)
                inverse[t] = jnp.broadcast_to(1.0 / l, (BLK, 128))

        def gather(i):
            for j in range(2):
                outs = []
                for half in range(2):
                    t = 4 * i + j + 2 * half
                    o = jnp.dot(
                        weights[t], keys_of(i, j + 2 * half), preferred_element_type=F32
                    )
                    outs.append(o * inverse[t])
                att_send[homes[i], 4 * j:4 * j + 4] = jnp.where(
                    low, pltpu.roll(outs[0], 64, 1), outs[1]
                ).astype(BF).reshape(4, 16, 128)

        def give_back(i):
            def send():
                remote(
                    att_send.at[homes[i]], att_recv.at[chip], att_ss, att_rs.at[g],
                    to_ctx(homes[i]),
                ).start()

            if i == OWN % STEP:
                pl.when(g != OWN // STEP)(send)
            else:
                send()

        for i in range(STEP):
            score(i)
        for i in range(STEP):
            soften(i)
        for i in range(STEP):
            gather(i)
        for i in range(STEP):
            give_back(i)

        return carry

    lax.fori_loop(0, GROUPS, attend, 0)
    pltpu.make_async_copy(att_send.at[chip], att_recv.at[chip], att_rs.at[GROUPS - 1]).start()

    tok_piece = jnp.zeros((8, 128), F32)
    for k in range(CHIPS):
        tok_piece = tok_piece + q_recv[k, 128:QROWS, :].astype(F32)
    att_piece = jnp.zeros((8, 128), F32)
    row8 = lax.broadcasted_iota(jnp.int32, (8, 1), 0)
    row16 = lax.broadcasted_iota(jnp.int32, (16, 1), 0)
    for d in range(DOCS):
        home = lax.div(starts[d], ROWS)
        local = lax.rem(starts[d], ROWS)
        packed = lax.rem(local, 128)
        tile = att_send[lax.div(home, 2), lax.div(packed, 16)].astype(F32)
        here = row16 + 16 * core == lax.rem(packed, 16) + 16 * lax.rem(home, 2)
        one = jnp.where(here, tile, 0.0)
        one = jnp.sum(one, axis=0, keepdims=True)
        one = jnp.where(lane * 0 + local >= 128, pltpu.roll(one, 64, 1), one)
        att_piece = jnp.where(row8 == d, one, att_piece)
    doc_send[...] = jnp.concatenate((att_piece, tok_piece), axis=0).astype(BF)
    near = remote(doc_send, doc_near, near_ss, near_rs, sibling)
    near.start()

    for n in range(2, 5):
        small_load(n).wait()

    def normed(rows):
        centre = jnp.mean(rows, axis=1, keepdims=True)
        spread = jnp.mean(jnp.square(rows - centre), axis=1, keepdims=True)
        return ((rows - centre) * lax.rsqrt(spread + 1e-05) * gain_ref[...] + bias_ref[...]).astype(BF)

    late_load(2).wait()
    def documents():
        drain(doc_recv, doc_rs)
        pieces = [doc_recv[h].astype(F32) for h in range(CHIPS)]
        opened = jnp.concatenate(
            [
                jnp.where(low, pieces[2 * j], pltpu.roll(pieces[2 * j + 1], 64, 1))
                for j in range(CHIPS // 2)
            ],
            axis=1,
        )
        y = jnp.dot(opened.astype(BF), wo[...], preferred_element_type=F32)
        doc_ref[...] = jnp.tanh(
            jnp.dot(normed(opened[8:] + y[:8]), wp[...], preferred_element_type=F32)
            + pbias_ref[...]
        )


    late_load(1).wait()
    for g in range(4):
        if g == 3:
            documents()
        drain(att_recv.at[pl.ds(0, 4)], att_rs.at[g])
        x = ahead_x[g]
        for p in range(2):
            even = att_recv[4 * x + 2 * p].reshape(128, 128).astype(F32)
            odd = att_recv[4 * x + 2 * p + 1].reshape(128, 128).astype(F32)
            top, bottom = interleave(even, odd)
            s = slice(128 * p, 128 * p + 128)
            lhs[0:128, s] = top.astype(BF)
            lhs[128:256, s] = bottom.astype(BF)
        heads = pl.ds(pl.multiple_of(x * 256, 256), 256)
        y = jnp.dot(lhs[...], wo[heads, :], preferred_element_type=F32)
        if g == 0:
            mixed[...] = tok_ref[...].astype(F32) + y
        else:
            mixed[...] = mixed[...] + y
        if g == 0:
            near.wait_recv()
            doc_sum[...] = (doc_send[...].astype(F32) + doc_near[...].astype(F32)).astype(BF)
            for k in others:
                doc_copy(k).start()
            pltpu.make_async_copy(doc_sum, doc_recv.at[chip], doc_rs).start()

    for n in range(8):
        rows = slice(32 * n, 32 * n + 32)
        enc_ref[rows, :] = normed(mixed[rows, :])

    most = pl.ds(0, CHIPS - 1)
    drain(ids_recv.at[most], ids_ss)
    drain(kv_send.at[most], kv_ss)
    drain(q_send.at[most], q_ss)
    drain(att_send.at[most], att_ss)
    drain(kv_send, sib_ss)
    near.wait_send()
    drain(doc_recv.at[most], doc_ss)


def per_device(
    tokens, w_query, w_key, w_value, w_out, norm_gain, norm_bias, w_pool, pool_bias,
    random_ids, lengths,
):
    vmem = pl.BlockSpec(memory_space=pltpu.VMEM)
    hbm = pl.BlockSpec(memory_space=pltpu.HBM)
    ids = random_ids.transpose(2, 0, 1)
    dma = pltpu.SemaphoreType.DMA
    return pl.pallas_call(
        kernel,
        out_shape=(
            jax.ShapeDtypeStruct((ROWS, D), BF),
            jax.ShapeDtypeStruct((DOCS, D), F32),
        ),
        in_specs=[hbm] * 11,
        out_specs=(vmem, vmem),
        scratch_shapes=[
            pltpu.VMEM((RAND, 4, HEADS), jnp.int32), pltpu.SMEM((DOCS,), jnp.int32),
            pltpu.VMEM((ROWS, D), BF),
            pltpu.VMEM((1, D), F32), pltpu.VMEM((1, D), F32), pltpu.VMEM((1, D), F32),
            pltpu.VMEM((D, D), BF), pltpu.VMEM((D, D), BF), pltpu.VMEM((D, D), BF),
            pltpu.VMEM((D, D), BF), pltpu.VMEM((D, D), BF),
            pltpu.VMEM((CHIPS, 4, BLK, 128), BF),
            pltpu.VMEM((NBLK + 2, BLK, 128), BF),
            pltpu.VMEM((CHIPS, QROWS, 128), BF),
            pltpu.VMEM((CHIPS, QROWS, 128), BF),
            pltpu.VMEM((CHIPS, 8, 16, 128), BF),
            pltpu.VMEM((CHIPS, 8, 16, 128), BF),
            pltpu.VMEM((16, 128), BF), pltpu.VMEM((16, 128), BF), pltpu.VMEM((16, 128), BF),
            pltpu.VMEM((CHIPS, 16, 128), BF),
            pltpu.VMEM((1, 256), jnp.int32),
            pltpu.VMEM((CHIPS, 1, 256), jnp.int32),
            pltpu.SMEM((CHIPS, 1, 256), jnp.int32),
            pltpu.VMEM((CHIPS * 4, BLK, 256), jnp.int32),
            pltpu.VMEM((4 * STEP, BLK, KEYS), F32),
            pltpu.VMEM((4 * STEP, BLK, KEYS), BF),
            pltpu.VMEM((4 * STEP, BLK, 128), F32),
            pltpu.VMEM((ROWS, 256), BF),
            pltpu.VMEM((ROWS, D), F32),
            dma((11,)), dma((9,)), dma, dma, dma, dma((CHIPS,)), dma, dma,
            dma, dma((GROUPS,)), dma, dma((GROUPS,)), dma, dma, dma, dma,
        ],
        compiler_params=pltpu.CompilerParams(
            collective_id=0, has_side_effects=True, vmem_limit_bytes=32 << 20
        ),
    )(*[
        pltpu.with_memory_space_constraint(x, pltpu.HBM)
        for x in (
            ids, lengths, tokens, norm_gain.reshape(1, D), norm_bias.reshape(1, D),
            pool_bias.reshape(1, D), w_query, w_key, w_value, w_out, w_pool,
        )
    ])


def solution(mesh):
    rows = P(("dp", "ctx"), None)
    placed = (
        rows, P(), P(), P(), P(), P(), P(), P(), P(),
        P(("dp", "ctx"), None, None), P("dp"),
    )
    return jax.shard_map(
        per_device,
        mesh=mesh,
        in_specs=placed,
        out_specs=(rows, P("dp", None)),
        check_vma=False,
    )
```
